32 devices in a mesh: dp: 4 (over y, x), eng: 2 (over core), tp: 4 (over z).
Axes of the slice: x: 2, y: 2, z: 4, core: 2. Of those that a mesh axis runs over, the one named last changes fastest.
Arguments:
- grad_parts: bfloat16 [4, 4, 1024, 14336], P('dp', 'tp', None, 'eng'), may hold values from -24 to 24
- master: float32 [4, 1024, 14336], P('tp', 'dp', 'eng'), may hold values from -0.09375 to 0.09375
- first_moment: float32 [4, 1024, 14336], P('tp', 'dp', 'eng'), may hold values from -12 to 12
- second_moment: float32 [4, 1024, 14336], P('tp', 'dp', 'eng'), may hold values from 4 to 256
- adam_step: int32 [1], replicated, may hold values from 1 to 999
- rank_map: int32 [4], replicated, may hold values from 0 to 3, each once
Outputs:
- new_master: float32 [4, 1024, 14336], P('tp', 'dp', 'eng')
- new_first: float32 [4, 1024, 14336], P('tp', 'dp', 'eng')
- new_second: float32 [4, 1024, 14336], P('tp', 'dp', 'eng')
- rollout: bfloat16 [4, 1024, 2, 4, 1792], P(None, 'dp', None, 'tp')
The draws below stay inside these ranges and needn't reach their ends.
Inputs may be any that keep to these rules, and one draw needn't show every extreme that they name: `rank_map`: each of 0 to 3 appears once.
All inputs are finite; a program needn't handle non-finite values.
Results may differ from the reference program's by a relative error of at most 0.001.
Values may be sent and summed in bfloat16 or wider, within the bound.
A program may use at most 192 MiB of HBM per device.

```python
import math
import jax
import jax.numpy as jnp
from jax import lax

D = 4096
F = 14336
N_DP = 4
N_ENG = 2
N_TP = 4


def with_spikes(drawn, key, source, target, parts, factor):
    def block_of(dim):
        return (jnp.arange(drawn.shape[dim]) // (drawn.shape[dim] // parts)).reshape((-1,) + (1,) * (drawn.ndim - 1 - dim))

    near = jax.random.permutation(key, parts)[block_of(target)]
    second = (block_of(target) + parts // 2) % parts
    return jnp.where((block_of(source) == near) | (block_of(source) == second), factor * drawn, drawn)


def shard_levels(rng, shape, split, low, high):
    loudness, own = 1.0, jax.random.fold_in(rng, 6)
    for dim, parts in split:
        steps = jnp.exp(jax.random.uniform(jax.random.fold_in(own, dim), (parts,), jnp.float32, low / len(split), high / len(split)))
        loudness = loudness * jnp.repeat(steps, shape[dim] // parts).reshape([-1 if axis == dim else 1 for axis in range(len(shape))])
    return loudness


def centred(rng, dims, width, limit, split=(), dtype=jnp.bfloat16):
    level = shard_levels(rng, dims, split, -0.22, 0.18) if split else 1.0
    drawn = jax.random.normal(rng, dims, jnp.float32) * width * level
    return jnp.minimum(jnp.maximum(drawn, -limit), limit).astype(dtype)


def heavy_noise(stream_key, dims, width, most, shards, heavy, kind=jnp.bfloat16):
    drawn = width * jax.random.normal(stream_key, dims, jnp.float32)
    if shards:
        drawn = drawn * shard_levels(stream_key, dims, shards, -0.22, 0.18)
    return jnp.clip(with_spikes(drawn, jax.random.fold_in(stream_key, 3), *heavy), -most, most).astype(kind)


def setup_inputs(seed: int = 0) -> dict:
    seeds = jax.random.split(jax.random.key(seed), 7)
    return {
        "grad_parts": heavy_noise(seeds[0], (N_DP, N_TP, D // N_TP, F), 4.0, 24.0, ((0, 4), (1, 4), (3, 2)), (0, 2, 4, 2.0)),
        "master": centred(seeds[1], (N_TP, D // N_TP, F), D ** -0.5, 0.09375, ((0, 4), (1, 4), (2, 2)), jnp.float32),
        "first_moment": centred(seeds[2], (N_TP, D // N_TP, F), 2.0, 12.0, ((0, 4), (1, 4), (2, 2)), jnp.float32),
        "second_moment": jnp.clip(jnp.exp(math.log(256.0) - 4.158883 * jax.random.uniform(seeds[3], (N_TP, D // N_TP, F), jnp.float32) ** shard_levels(seeds[3], (N_TP, D // N_TP, F), ((0, 4), (1, 4), (2, 2)), -0.2, 0.2)), 4.0, 256.0),
        "adam_step": jax.random.randint(seeds[4], (1,), 1, 1000).astype(jnp.int32),
        "rank_map": jax.random.permutation(seeds[5], N_TP).astype(jnp.int32),
    }


beta_one = 0.9
beta_two = 0.95
rate_value = 0.001
decay_value = 0.01
eps_value = 1e-08

def reference(grad_parts, master, first_moment, second_moment, adam_step, rank_map):
    summed = lax.optimization_barrier(jnp.sum(grad_parts.astype(jnp.float32), axis=0))
    count = adam_step[0].astype(jnp.float32)
    new_first = beta_one * first_moment + (1.0 - beta_one) * summed
    new_second = beta_two * second_moment + (1.0 - beta_two) * summed * summed
    first_hat = new_first / (1.0 - jnp.power(beta_one, count))
    second_hat = new_second / (1.0 - jnp.power(beta_two, count))
    new_master = master - rate_value * (first_hat / (jnp.sqrt(second_hat) + eps_value) + decay_value * master)
    weights = new_master.astype(jnp.bfloat16).reshape(N_TP, D // N_TP, N_ENG, N_TP, F // (N_ENG * N_TP))
    rollout = jnp.take(weights, rank_map.astype(jnp.int32), axis=3)
    return (new_master, new_first, new_second, rollout)
```

```python
import functools
import jax
import jax.numpy as jnp
from jax import lax
from jax.experimental import pallas as pl
from jax.experimental.pallas import tpu as pltpu
from jax.sharding import PartitionSpec as P

beta_one = 0.9
beta_two = 0.95
rate_value = 0.001
decay_value = 0.01
eps_value = 1e-08

ROWS = 16
AHEAD = 3
STRIP = 256
TOP = 32767.0
TINY = 1e-30
MESH = pl.DeviceIdType.MESH


def corrections(adam_step):
    count = adam_step[0].astype(jnp.float32)
    return 1.0 - jnp.power(beta_one, count), 1.0 - jnp.power(beta_two, count)


def plain_shards(grad_parts, master, first_moment, second_moment, adam_step, rank_map):
    summed = lax.psum_scatter(grad_parts.astype(jnp.float32), "dp", scatter_dimension=2, tiled=True)
    summed = summed.reshape(master.shape)
    fix_one, fix_two = corrections(adam_step)
    new_first = beta_one * first_moment + (1.0 - beta_one) * summed
    new_second = beta_two * second_moment + (1.0 - beta_two) * summed * summed
    first_hat = new_first / fix_one
    second_hat = new_second / fix_two
    new_master = master - rate_value * (
        first_hat / (jnp.sqrt(second_hat) + eps_value) + decay_value * master
    )
    row_count = master.shape[1]
    ranks = lax.axis_size("tp")
    block_width = master.shape[2] // ranks
    piece = new_master.astype(jnp.bfloat16).reshape(1, row_count, 1, ranks, block_width)
    ordered = jnp.take(piece, rank_map, axis=3)
    placed = lax.all_to_all(ordered, "tp", split_axis=3, concat_axis=0, tiled=True)
    rollout = lax.all_gather(placed, "eng", axis=2, tiled=True)
    return (new_master, new_first, new_second, rollout)


def pack_sum(near, far, packed, scale):
    tiles = packed.shape[1] // 128
    tops = [jnp.zeros((8, 128), jnp.float32) for _ in range(4)]
    for tile in range(tiles):
        columns = pl.ds(tile * 128, 128)
        size = jnp.abs(near[:, columns].astype(jnp.float32) + far[:, columns].astype(jnp.float32))
        for part in range(ROWS // 8):
            slot = (2 * tile + part) % 4
            tops[slot] = jnp.maximum(tops[slot], size[8 * part : 8 * part + 8])
    top = jnp.maximum(jnp.maximum(tops[0], tops[1]), jnp.maximum(tops[2], tops[3]))
    top = jnp.maximum(top, TINY)
    scale[...] = top * (1.0 / TOP)
    factor = jnp.concatenate([TOP / top] * (ROWS // 8), axis=0)
    for tile in range(tiles):
        columns = pl.ds(tile * 128, 128)
        value = near[:, columns].astype(jnp.float32) + far[:, columns].astype(jnp.float32)
        packed[:, columns] = jnp.round(value * factor).astype(jnp.int32).astype(jnp.int16)


def kernel(
    ranks, order, scales, grad, master, first, second,
    new_master, new_first, new_second, both,
    rxa, rxb, txa, txb, tsa, tsb, r2a, r2b, rsa, rsb, zs, zr,
    own, side_a, side_b, old, new, held,
    p1_send, p1_recv, p2_send, p2_recv, z_send, z_recv, f_send, f_recv,
    own_sem, side_sem, old_sem, new_sem, keep_sem,
):
    columns = grad.shape[2]
    half = columns // 2
    width = columns // ranks
    chunks = rxa.shape[0]
    me, tp, eng = (lax.axis_index(a) for a in ("dp", "tp", "eng"))
    at_x = me + 1 - 2 * (me % 2)
    at_y = (me + 2) % 4
    at_d = 3 - me
    left, right = pl.ds(0, half), pl.ds(half, half)
    states, outs = (master, first, second), (new_master, new_first, new_second)

    def rows_of(chunk):
        return pl.ds(pl.multiple_of(chunk * ROWS, ROWS), ROWS)

    def remote(src, dst, send, recv, **where):
        return pltpu.make_async_remote_copy(
            src_ref=src, dst_ref=dst, send_sem=send, recv_sem=recv, device_id=where, device_id_type=MESH
        )

    def first_stage(c):
        rows = rows_of(c)
        return [
            remote(grad.at[at_d, rows, left], rxa.at[c, 1], p1_send.at[c, 0], p1_recv.at[c, 0], dp=at_x),
            remote(grad.at[at_d, rows, right], rxb.at[c, 1], p1_send.at[c, 1], p1_recv.at[c, 1], dp=at_y),
            remote(grad.at[at_x, rows, left], rxa.at[c, 0], p1_send.at[c, 2], p1_recv.at[c, 2], dp=at_x),
            remote(grad.at[at_y, rows, right], rxb.at[c, 0], p1_send.at[c, 3], p1_recv.at[c, 3], dp=at_y),
        ]

    def second_stage(c):
        return [
            remote(txa.at[c], r2a.at[c], p2_send.at[c, 0], p2_recv.at[c, 0], dp=at_y),
            remote(tsa.at[c], rsa.at[c], p2_send.at[c, 1], p2_recv.at[c, 1], dp=at_y),
            remote(txb.at[c], r2b.at[c], p2_send.at[c, 2], p2_recv.at[c, 2], dp=at_x),
            remote(tsb.at[c], rsb.at[c], p2_send.at[c, 3], p2_recv.at[c, 3], dp=at_x),
        ]

    def publish(c):
        return [
            remote(zs.at[c, hop], zr.at[hop, c], z_send.at[c, hop], z_recv.at[c, hop], tp=(tp + hop) % ranks)
            for hop in range(1, ranks)
        ]

    def forward(c, hop):
        src = zs.at[c, 0] if hop == 0 else zr.at[hop, c]
        place = both.at[eng, (tp + ranks - hop) % ranks, rows_of(c)]
        return (
            remote(src, place, f_send.at[c, hop], f_recv.at[c, hop], eng=1 - eng),
            pltpu.make_async_copy(src, place, keep_sem.at[c, hop]),
        )

    def arrived(c, hop):
        place = both.at[1 - eng, (tp + ranks - hop) % ranks, rows_of(c)]
        return remote(place, place, f_send.at[c, hop], f_recv.at[c, hop], eng=1 - eng)

    def load_own(c):
        return [pltpu.make_async_copy(grad.at[me, rows_of(c)], own.at[c % 2], own_sem.at[c % 2])]

    def load_side(c):
        return [
            pltpu.make_async_copy(grad.at[at_y, rows_of(c), left], side_a.at[c % 2], side_sem.at[c % 2, 0]),
            pltpu.make_async_copy(grad.at[at_x, rows_of(c), right], side_b.at[c % 2], side_sem.at[c % 2, 1]),
        ]

    def load_old(c):
        return [
            pltpu.make_async_copy(states[i].at[rows_of(c)], old.at[c % 2, i], old_sem.at[c % 2, i]) for i in range(3)
        ]

    def store_new(c):
        return [
            pltpu.make_async_copy(new.at[c % 2, i], outs[i].at[rows_of(c)], new_sem.at[c % 2, i]) for i in range(3)
        ]

    def start(copies):
        for copy in copies:
            copy.start()

    def wait(copies):
        for copy in copies:
            copy.wait()

    def wait_recv(copies):
        for copy in copies:
            copy.wait_recv()

    for c in range(2):
        start(load_side(c) + load_own(c) + load_old(c))
    barrier = pltpu.get_barrier_semaphore()
    for where in (
        [{"dp": at_x}, {"dp": at_y}, {"eng": 1 - eng}] + [{"tp": (tp + hop) % ranks} for hop in range(1, ranks)]
    ):
        pl.semaphore_signal(barrier, inc=1, device_id=where, device_id_type=MESH)
    pl.semaphore_wait(barrier, 2 + ranks)
    for c in range(AHEAD):
        start(first_stage(c))

    def reduce_side(c):
        slot = c % 2
        wait(load_side(c))
        copies = first_stage(c)
        copies[0].wait_recv()
        pack_sum(side_a.at[slot], rxa.at[c, 1], txa.at[c], tsa.at[c])
        start(second_stage(c)[:2])
        copies[1].wait_recv()
        pack_sum(side_b.at[slot], rxb.at[c, 1], txb.at[c], tsb.at[c])
        start(second_stage(c)[2:])

        @pl.when(c + 2 < chunks)
        def _():
            start(load_side(c + 2))

    def update(c):
        slot = c % 2
        wait(load_own(c) + load_old(c))
        wait_recv(first_stage(c)[2:])
        wait_recv(second_stage(c))

        @pl.when(c >= 2)
        def _():
            wait(store_new(c - 2))

        scale_one, scale_two = scales[0], scales[1]
        for strip in range(columns // STRIP):
            at = pl.ds(strip * STRIP, STRIP)
            side = strip * STRIP // half
            inner = pl.ds(strip * STRIP - side * half, STRIP)
            got, sums, units = ((rxa, r2a, rsa), (rxb, r2b, rsb))[side]
            unit = units[c]
            unit = jnp.concatenate([jnp.concatenate([unit] * (ROWS // 8), axis=0)] * (STRIP // 128), axis=1)
            summed = own[slot, :, at].astype(jnp.float32) + got[c, 0, :, inner].astype(jnp.float32)
            summed += sums[c, :, inner].astype(jnp.int32).astype(jnp.float32) * unit
            first_now = beta_one * old[slot, 1, :, at] + (1.0 - beta_one) * summed
            second_now = beta_two * old[slot, 2, :, at] + (1.0 - beta_two) * summed * summed
            was = old[slot, 0, :, at]
            step = (first_now * scale_one) / (jnp.sqrt(second_now * scale_two) + eps_value)
            now = was - rate_value * (step + decay_value * was)
            new[slot, 0, :, at] = now
            new[slot, 1, :, at] = first_now
            new[slot, 2, :, at] = second_now
            block = strip * STRIP // width
            held[block, :, pl.ds(strip * STRIP - block * width, STRIP)] = now.astype(jnp.bfloat16)
        start(store_new(c))
        for hop in range(ranks):
            zs[c, hop] = held[order[hop]]
        start(publish(c))
        start(forward(c, 0))

        @pl.when(c + 2 < chunks)
        def _():
            start(load_own(c + 2) + load_old(c + 2))

    def spread(c):
        copies = publish(c)
        for hop in range(1, ranks):
            copies[hop - 1].wait_recv()
            start(forward(c, hop))

    def body(s, carry):
        @pl.when(s + AHEAD < chunks)
        def _():
            start(first_stage(s + AHEAD))

        @pl.when(s < chunks)
        def _():
            reduce_side(s)

        @pl.when((s >= 1) & (s <= chunks))
        def _():
            update(s - 1)

        @pl.when(s >= 2)
        def _():
            spread(s - 2)

        return carry

    lax.fori_loop(0, chunks + 2, body, 0)

    def drain(c, carry):
        for copy in first_stage(c) + second_stage(c) + publish(c):
            copy.wait_send()
        for hop in range(ranks):
            away, keep = forward(c, hop)
            away.wait_send()
            keep.wait()
            arrived(c, hop).wait_recv()
        return carry

    lax.fori_loop(0, chunks, drain, 0)
    wait(store_new(chunks - 2) + store_new(chunks - 1))


def shards(grad_parts, master, first_moment, second_moment, adam_step, rank_map):
    replicas, ranks = lax.axis_size("dp"), lax.axis_size("tp")
    row_count, columns = master.shape[1], master.shape[2]
    half, width = columns // 2, columns // ranks
    chunks = row_count // ROWS
    me_tp = lax.axis_index("tp")
    grad = grad_parts.reshape(replicas, row_count, columns)
    states = [s.reshape(row_count, columns) for s in (master, first_moment, second_moment)]
    order = lax.dynamic_slice(jnp.concatenate([rank_map, rank_map]), (me_tp,), (ranks,))
    scales = jnp.stack([1.0 / value for value in corrections(adam_step)])
    smem, anywhere = pl.BlockSpec(memory_space=pltpu.SMEM), pl.BlockSpec(memory_space=pl.ANY)
    vmem, dma = pltpu.VMEM, pltpu.SemaphoreType.DMA
    short, brain, single = jnp.int16, jnp.bfloat16, jnp.float32
    *outs, both = pl.pallas_call(
        functools.partial(kernel, ranks),
        out_shape=[jax.ShapeDtypeStruct(s.shape, s.dtype) for s in states]
        + [jax.ShapeDtypeStruct((2, ranks, row_count, width), brain)],
        in_specs=[smem, smem] + [anywhere] * 4,
        out_specs=[anywhere] * 4,
        scratch_shapes=[
            vmem((chunks, 2, ROWS, half), brain),
            vmem((chunks, 2, ROWS, half), brain),
            vmem((chunks, ROWS, half), short),
            vmem((chunks, ROWS, half), short),
            vmem((chunks, 8, 128), single),
            vmem((chunks, 8, 128), single),
            vmem((chunks, ROWS, half), short),
            vmem((chunks, ROWS, half), short),
            vmem((chunks, 8, 128), single),
            vmem((chunks, 8, 128), single),
            vmem((chunks, ranks, ROWS, width), brain),
            vmem((ranks, chunks, ROWS, width), brain),
            vmem((2, ROWS, columns), brain),
            vmem((2, ROWS, half), brain),
            vmem((2, ROWS, half), brain),
            vmem((2, 3, ROWS, columns), single),
            vmem((2, 3, ROWS, columns), single),
            vmem((ranks, ROWS, width), brain),
            dma((chunks, 4)),
            dma((chunks, 4)),
            dma((chunks, 4)),
            dma((chunks, 4)),
            dma((chunks, ranks)),
            dma((chunks, ranks)),
            dma((chunks, ranks)),
            dma((chunks, ranks)),
            dma((2,)),
            dma((2, 2)),
            dma((2, 3)),
            dma((2, 3)),
            dma((chunks, ranks)),
        ],
        compiler_params=pltpu.CompilerParams(
            collective_id=0, has_side_effects=True, vmem_limit_bytes=48 * 1024 * 1024
        ),
        name="exchange",
    )(order, scales, grad, *states)
    rollout = jnp.transpose(both, (1, 2, 0, 3)).reshape(ranks, row_count, 2, 1, width)
    return (*(o.reshape(master.shape) for o in outs), rollout)


def solution(mesh):
    sizes = dict(mesh.shape)

    def step(grad_parts, master, *rest):
        columns = master.shape[2] // sizes["eng"]
        width = columns // sizes["tp"]
        rows = master.shape[1] // sizes["dp"]
        fits = sizes["dp"] == 4 and sizes["eng"] == 2 and width % STRIP == 0 and (columns // 2) % STRIP == 0
        fits = fits and rows % ROWS == 0 and rows // ROWS > AHEAD
        return jax.shard_map(
            shards if fits else plain_shards,
            mesh=mesh,
            in_specs=(
                P("dp", "tp", None, "eng"),
                P("tp", "dp", "eng"),
                P("tp", "dp", "eng"),
                P("tp", "dp", "eng"),
                P(),
                P(),
            ),
            out_specs=(
                P("tp", "dp", "eng"),
                P("tp", "dp", "eng"),
                P("tp", "dp", "eng"),
                P(None, "dp", None, "tp", None),
            ),
            check_vma=False,
        )(grad_parts, master, *rest)

    return step
```

```python
import functools
import jax
import jax.numpy as jnp
from jax import lax
from jax.experimental import pallas as pl
from jax.experimental.pallas import tpu as pltpu
from jax.sharding import PartitionSpec as P

beta_one = 0.9
beta_two = 0.95
rate_value = 0.001
decay_value = 0.01
eps_value = 1e-08

ROWS = 16
AHEAD = 2
STRIP = 256
TOP = 32767.0
TINY = 1e-30
MESH = pl.DeviceIdType.MESH


def corrections(adam_step):
    count = adam_step[0].astype(jnp.float32)
    return 1.0 - jnp.power(beta_one, count), 1.0 - jnp.power(beta_two, count)


def plain_shards(grad_parts, master, first_moment, second_moment, adam_step, rank_map):
    summed = lax.psum_scatter(grad_parts.astype(jnp.float32), "dp", scatter_dimension=2, tiled=True)
    summed = summed.reshape(master.shape)
    fix_one, fix_two = corrections(adam_step)
    new_first = beta_one * first_moment + (1.0 - beta_one) * summed
    new_second = beta_two * second_moment + (1.0 - beta_two) * summed * summed
    first_hat = new_first / fix_one
    second_hat = new_second / fix_two
    new_master = master - rate_value * (
        first_hat / (jnp.sqrt(second_hat) + eps_value) + decay_value * master
    )
    row_count = master.shape[1]
    ranks = lax.axis_size("tp")
    block_width = master.shape[2] // ranks
    piece = new_master.astype(jnp.bfloat16).reshape(1, row_count, 1, ranks, block_width)
    ordered = jnp.take(piece, rank_map, axis=3)
    placed = lax.all_to_all(ordered, "tp", split_axis=3, concat_axis=0, tiled=True)
    rollout = lax.all_gather(placed, "eng", axis=2, tiled=True)
    return (new_master, new_first, new_second, rollout)


def pack_sum(near, far, packed, scale):
    tiles = packed.shape[1] // 128
    tops = [jnp.zeros((8, 128), jnp.float32) for _ in range(4)]
    for tile in range(tiles):
        columns = pl.ds(tile * 128, 128)
        size = jnp.abs(near[:, columns].astype(jnp.float32) + far[:, columns].astype(jnp.float32))
        for part in range(ROWS // 8):
            slot = (2 * tile + part) % 4
            tops[slot] = jnp.maximum(tops[slot], size[8 * part : 8 * part + 8])
    top = jnp.maximum(jnp.maximum(tops[0], tops[1]), jnp.maximum(tops[2], tops[3]))
    top = jnp.maximum(top, TINY)
    scale[...] = top * (1.0 / TOP)
    factor = jnp.concatenate([TOP / top] * (ROWS // 8), axis=0)
    for tile in range(tiles):
        columns = pl.ds(tile * 128, 128)
        value = near[:, columns].astype(jnp.float32) + far[:, columns].astype(jnp.float32)
        packed[:, columns] = jnp.round(value * factor).astype(jnp.int32).astype(jnp.int16)


def kernel(
    ranks, order, scales, grad, master, first, second,
    new_master, new_first, new_second, rollout,
    rxa, rxb, txa, txb, tsa, tsb, r2a, r2b, rsa, rsb, zs, zr,
    own, side_a, side_b, old, held,
    p1_send, p1_recv, p2_send, p2_recv, z_send, z_recv, f_send, f_recv,
    own_sem, side_sem, old_sem,
):
    columns = grad.shape[2]
    half = columns // 2
    width = columns // ranks
    chunks = rxa.shape[0]
    me, tp, eng = (lax.axis_index(a) for a in ("dp", "tp", "eng"))
    at_x = me + 1 - 2 * (me % 2)
    at_y = (me + 2) % 4
    at_d = 3 - me
    left, right = pl.ds(0, half), pl.ds(half, half)
    states = (master, first, second)

    def rows_of(chunk):
        return pl.ds(pl.multiple_of(chunk * ROWS, ROWS), ROWS)

    def remote(src, dst, send, recv, **where):
        return pltpu.make_async_remote_copy(
            src_ref=src, dst_ref=dst, send_sem=send, recv_sem=recv, device_id=where, device_id_type=MESH
        )

    def first_stage(c):
        rows = rows_of(c)
        return [
            remote(grad.at[at_d, rows, left], rxa.at[c, 1], p1_send.at[c, 0], p1_recv.at[c, 0], dp=at_x),
            remote(grad.at[at_d, rows, right], rxb.at[c, 1], p1_send.at[c, 1], p1_recv.at[c, 1], dp=at_y),
            remote(grad.at[at_x, rows, left], rxa.at[c, 0], p1_send.at[c, 2], p1_recv.at[c, 2], dp=at_x),
            remote(grad.at[at_y, rows, right], rxb.at[c, 0], p1_send.at[c, 3], p1_recv.at[c, 3], dp=at_y),
        ]

    def second_stage(c):
        return [
            remote(txa.at[c], r2a.at[c], p2_send.at[c, 0], p2_recv.at[c, 0], dp=at_y),
            remote(tsa.at[c], rsa.at[c], p2_send.at[c, 1], p2_recv.at[c, 1], dp=at_y),
            remote(txb.at[c], r2b.at[c], p2_send.at[c, 2], p2_recv.at[c, 2], dp=at_x),
            remote(tsb.at[c], rsb.at[c], p2_send.at[c, 3], p2_recv.at[c, 3], dp=at_x),
        ]

    def publish(c, hop):
        return remote(
            zs.at[c, hop - 1], zr.at[eng, hop, c], z_send.at[c, hop], z_recv.at[c, hop], tp=(tp + hop) % ranks
        )

    def forward(c, hop):
        block = zr.at[eng, hop, c]
        return remote(block, block, f_send.at[c, hop], f_recv.at[c, hop], eng=1 - eng)

    def arrival(c, hop):
        block = zr.at[1 - eng, hop, c]
        return remote(block, block, f_send.at[c, hop], f_recv.at[c, hop], eng=1 - eng)

    def load_own(c):
        return [pltpu.make_async_copy(grad.at[me, rows_of(c)], own.at[c % 2], own_sem.at[c % 2])]

    def load_side(c):
        return [
            pltpu.make_async_copy(grad.at[at_y, rows_of(c), left], side_a.at[c % 2], side_sem.at[c % 2, 0]),
            pltpu.make_async_copy(grad.at[at_x, rows_of(c), right], side_b.at[c % 2], side_sem.at[c % 2, 1]),
        ]

    def load_old(c):
        return [
            pltpu.make_async_copy(states[i].at[rows_of(c)], old.at[c % 2, i], old_sem.at[c % 2, i]) for i in range(3)
        ]

    def start(copies):
        for copy in copies:
            copy.start()

    def wait(copies):
        for copy in copies:
            copy.wait()

    def wait_recv(copies):
        for copy in copies:
            copy.wait_recv()

    for c in range(2):
        start(load_side(c) + load_own(c) + load_old(c))
    barrier = pltpu.get_barrier_semaphore()
    for where in (
        [{"dp": at_x}, {"dp": at_y}, {"eng": 1 - eng}] + [{"tp": (tp + hop) % ranks} for hop in range(1, ranks)]
    ):
        pl.semaphore_signal(barrier, inc=1, device_id=where, device_id_type=MESH)
    pl.semaphore_wait(barrier, 2 + ranks)
    for c in range(AHEAD):
        start(first_stage(c))

    def reduce_side(c):
        slot = c % 2
        wait(load_side(c))
        copies = first_stage(c)
        copies[0].wait_recv()
        pack_sum(side_a.at[slot], rxa.at[c, 1], txa.at[c], tsa.at[c])
        start(second_stage(c)[:2])
        copies[1].wait_recv()
        pack_sum(side_b.at[slot], rxb.at[c, 1], txb.at[c], tsb.at[c])
        start(second_stage(c)[2:])

        @pl.when(c + 2 < chunks)
        def _():
            start(load_side(c + 2))

    def update(c):
        slot, rows = c % 2, rows_of(c)
        wait(load_own(c) + load_old(c))
        wait_recv(first_stage(c)[2:])
        wait_recv(second_stage(c))

        scale_one, scale_two = scales[0], scales[1]
        for strip in range(columns // STRIP):
            at = pl.ds(strip * STRIP, STRIP)
            side = strip * STRIP // half
            inner = pl.ds(strip * STRIP - side * half, STRIP)
            got, sums, units = ((rxa, r2a, rsa), (rxb, r2b, rsb))[side]
            unit = units[c]
            unit = jnp.concatenate([jnp.concatenate([unit] * (ROWS // 8), axis=0)] * (STRIP // 128), axis=1)
            summed = own[slot, :, at].astype(jnp.float32) + got[c, 0, :, inner].astype(jnp.float32)
            summed += sums[c, :, inner].astype(jnp.int32).astype(jnp.float32) * unit
            first_now = beta_one * old[slot, 1, :, at] + (1.0 - beta_one) * summed
            second_now = beta_two * old[slot, 2, :, at] + (1.0 - beta_two) * summed * summed
            was = old[slot, 0, :, at]
            step = (first_now * scale_one) / (jnp.sqrt(second_now * scale_two) + eps_value)
            now = was - rate_value * (step + decay_value * was)
            new_master[rows, at] = now
            new_first[rows, at] = first_now
            new_second[rows, at] = second_now
            block = strip * STRIP // width
            held[block, :, pl.ds(strip * STRIP - block * width, STRIP)] = now.astype(jnp.bfloat16)
        for hop in range(1, ranks):
            zs[c, hop - 1] = held[order[hop]]
            publish(c, hop).start()
        zr[eng, 0, c] = held[order[0]]
        forward(c, 0).start()

        @pl.when(c + 2 < chunks)
        def _():
            start(load_own(c + 2) + load_old(c + 2))

    def spread(c):
        for hop in range(1, ranks):
            publish(c, hop).wait_recv()
            forward(c, hop).start()

    def merge(c):
        for hop in range(ranks):
            arrival(c, hop).wait_recv()
            rollout[(tp + ranks - hop) % ranks, rows_of(c), 0, :] = zr[0, hop, c]
            rollout[(tp + ranks - hop) % ranks, rows_of(c), 1, :] = zr[1, hop, c]

    def body(s, carry):
        @pl.when(s + AHEAD < chunks)
        def _():
            start(first_stage(s + AHEAD))

        @pl.when(s < chunks)
        def _():
            reduce_side(s)

        @pl.when((s >= 1) & (s <= chunks))
        def _():
            update(s - 1)

        @pl.when((s >= 2) & (s < chunks + 2))
        def _():
            spread(s - 2)

        @pl.when(s >= 3)
        def _():
            merge(s - 3)

        return carry

    lax.fori_loop(0, chunks + 3, body, 0)

    def drain(c, carry):
        for copy in first_stage(c) + second_stage(c) + [publish(c, hop) for hop in range(1, ranks)]:
            copy.wait_send()
        for hop in range(ranks):
            forward(c, hop).wait_send()
        return carry

    lax.fori_loop(0, chunks, drain, 0)


def flush(*refs):
    count = (len(refs) - 1) // 2
    copies = [pltpu.make_async_copy(refs[i], refs[count + i], refs[-1].at[i]) for i in range(count)]
    for copy in copies:
        copy.start()
    for copy in copies:
        copy.wait()


def shards(grad_parts, master, first_moment, second_moment, adam_step, rank_map):
    replicas, ranks = lax.axis_size("dp"), lax.axis_size("tp")
    row_count, columns = master.shape[1], master.shape[2]
    half, width = columns // 2, columns // ranks
    chunks = row_count // ROWS
    me_tp = lax.axis_index("tp")
    grad = grad_parts.reshape(replicas, row_count, columns)
    states = [s.reshape(row_count, columns) for s in (master, first_moment, second_moment)]
    order = lax.dynamic_slice(jnp.concatenate([rank_map, rank_map]), (me_tp,), (ranks,))
    scales = jnp.stack([1.0 / value for value in corrections(adam_step)])
    smem, anywhere = pl.BlockSpec(memory_space=pltpu.SMEM), pl.BlockSpec(memory_space=pl.ANY)
    vmem, dma = pltpu.VMEM, pltpu.SemaphoreType.DMA
    short, brain, single = jnp.int16, jnp.bfloat16, jnp.float32
    held = [vmem(s.shape, s.dtype) for s in states] + [vmem((ranks, row_count, 2, width), brain)]
    results = pl.pallas_call(
        functools.partial(kernel, ranks),
        out_shape=held,
        in_specs=[smem, smem] + [anywhere] * 4,
        out_specs=[pl.BlockSpec(memory_space=pltpu.VMEM)] * 4,
        scratch_shapes=[
            vmem((chunks, 2, ROWS, half), brain),
            vmem((chunks, 2, ROWS, half), brain),
            vmem((chunks, ROWS, half), short),
            vmem((chunks, ROWS, half), short),
            vmem((chunks, 8, 128), single),
            vmem((chunks, 8, 128), single),
            vmem((chunks, ROWS, half), short),
            vmem((chunks, ROWS, half), short),
            vmem((chunks, 8, 128), single),
            vmem((chunks, 8, 128), single),
            vmem((chunks, ranks - 1, ROWS, width), brain),
            vmem((2, ranks, chunks, ROWS, width), brain),
            vmem((2, ROWS, columns), brain),
            vmem((2, ROWS, half), brain),
            vmem((2, ROWS, half), brain),
            vmem((2, 3, ROWS, columns), single),
            vmem((ranks, ROWS, width), brain),
            dma((chunks, 4)),
            dma((chunks, 4)),
            dma((chunks, 4)),
            dma((chunks, 4)),
            dma((chunks, ranks)),
            dma((chunks, ranks)),
            dma((chunks, ranks)),
            dma((chunks, ranks)),
            dma((2,)),
            dma((2, 2)),
            dma((2, 3)),
        ],
        compiler_params=pltpu.CompilerParams(
            collective_id=0, has_side_effects=True, vmem_limit_bytes=32 * 1024 * 1024
        ),
        name="exchange",
    )(order, scales, grad, *states)
    *outs, rollout = pl.pallas_call(
        flush,
        out_shape=[jax.ShapeDtypeStruct(r.shape, r.dtype) for r in results],
        in_specs=[anywhere] * 4,
        out_specs=[anywhere] * 4,
        scratch_shapes=[dma((4,))],
        compiler_params=pltpu.CompilerParams(vmem_limit_bytes=1024 * 1024),
        name="flush",
    )(*results)
    return (*(o.reshape(master.shape) for o in outs), rollout.reshape(ranks, row_count, 2, 1, width))


def solution(mesh):
    sizes = dict(mesh.shape)

    def step(grad_parts, master, *rest):
        columns = master.shape[2] // sizes["eng"]
        width = columns // sizes["tp"]
        rows = master.shape[1] // sizes["dp"]
        fits = sizes["dp"] == 4 and sizes["eng"] == 2 and width % STRIP == 0 and (columns // 2) % STRIP == 0
        fits = fits and rows % ROWS == 0 and rows // ROWS > AHEAD
        return jax.shard_map(
            shards if fits else plain_shards,
            mesh=mesh,
            in_specs=(
                P("dp", "tp", None, "eng"),
                P("tp", "dp", "eng"),
                P("tp", "dp", "eng"),
                P("tp", "dp", "eng"),
                P(),
                P(),
            ),
            out_specs=(
                P("tp", "dp", "eng"),
                P("tp", "dp", "eng"),
                P("tp", "dp", "eng"),
                P(None, "dp", None, "tp", None),
            ),
            check_vma=False,
        )(grad_parts, master, *rest)

    return step
```

```python
import functools
import math
import types
import jax
import jax.numpy as jnp
from jax import lax
from jax.experimental import pallas as pl
from jax.experimental.pallas import tpu as pltpu
from jax.sharding import PartitionSpec as P

beta_one = 0.9
beta_two = 0.95
rate_value = 0.001
decay_value = 0.01
eps_value = 1e-08

ROWS = 16
TAIL = 8
FAR, NEAR = 2, 1
UPDATE, SPREAD, MERGE = 1, 3, 4
STRIP = 256
TOP = 32767.0
TINY = 1e-30
MESH = pl.DeviceIdType.MESH


def corrections(adam_step):
    count = adam_step[0].astype(jnp.float32)
    return 1.0 - jnp.power(beta_one, count), 1.0 - jnp.power(beta_two, count)


def plain_shards(grad_parts, master, first_moment, second_moment, adam_step, rank_map):
    summed = lax.psum_scatter(grad_parts.astype(jnp.float32), "dp", scatter_dimension=2, tiled=True)
    summed = summed.reshape(master.shape)
    fix_one, fix_two = corrections(adam_step)
    new_first = beta_one * first_moment + (1.0 - beta_one) * summed
    new_second = beta_two * second_moment + (1.0 - beta_two) * summed * summed
    first_hat = new_first / fix_one
    second_hat = new_second / fix_two
    new_master = master - rate_value * (
        first_hat / (jnp.sqrt(second_hat) + eps_value) + decay_value * master
    )
    row_count = master.shape[1]
    ranks = lax.axis_size("tp")
    block_width = master.shape[2] // ranks
    piece = new_master.astype(jnp.bfloat16).reshape(1, row_count, 1, ranks, block_width)
    ordered = jnp.take(piece, rank_map, axis=3)
    placed = lax.all_to_all(ordered, "tp", split_axis=3, concat_axis=0, tiled=True)
    rollout = lax.all_gather(placed, "eng", axis=2, tiled=True)
    return (new_master, new_first, new_second, rollout)


def stacked(value, times, axis):
    return jnp.concatenate([value] * times, axis=axis) if times > 1 else value


def pack_sum(near, far, packed, scale):
    rows, tiles = packed.shape[0], packed.shape[1] // 128
    tops = [jnp.zeros((8, 128), jnp.float32) for _ in range(4)]
    for tile in range(tiles):
        columns = pl.ds(tile * 128, 128)
        size = jnp.abs(near[:, columns].astype(jnp.float32) + far[:, columns].astype(jnp.float32))
        for part in range(rows // 8):
            slot = (2 * tile + part) % 4
            tops[slot] = jnp.maximum(tops[slot], size[8 * part : 8 * part + 8])
    top = jnp.maximum(jnp.maximum(tops[0], tops[1]), jnp.maximum(tops[2], tops[3]))
    top = jnp.maximum(jnp.max(top, axis=0, keepdims=True), TINY)
    scale[...] = top * (1.0 / TOP)
    factor = jnp.broadcast_to(TOP / top, (rows, 128))
    for tile in range(tiles):
        columns = pl.ds(tile * 128, 128)
        value = near[:, columns].astype(jnp.float32) + far[:, columns].astype(jnp.float32)
        packed[:, columns] = jnp.round(value * factor).astype(jnp.int32).astype(jnp.int16)


def kernel(ranks, names, rank_map, adam_step, grad, master, first, second, *refs):
    new_master, new_first, new_second, rollout = refs[:4]
    body_refs, tail_refs = refs[4 : 4 + len(names)], refs[4 + len(names) :]
    columns = grad.shape[2]
    half = columns // 2
    width = columns // ranks
    me, tp, eng = (lax.axis_index(a) for a in ("dp", "tp", "eng"))
    at_x = me + 1 - 2 * (me % 2)
    at_y = (me + 2) % 4
    at_d = 3 - me
    barrier = pltpu.get_barrier_semaphore()
    for where in (
        [{"dp": at_x}, {"dp": at_y}, {"eng": 1 - eng}] + [{"tp": (tp + hop) % ranks} for hop in range(1, ranks)]
    ):
        pl.semaphore_signal(barrier, inc=1, device_id=where, device_id_type=MESH)
    left, right = pl.ds(0, half), pl.ds(half, half)
    states = (master, first, second)
    main = types.SimpleNamespace(**dict(zip(names, body_refs)), base=0, start=0)
    main.chunks, main.rows = main.rxa.shape[0], main.rxa.shape[2]
    tail = types.SimpleNamespace(**dict(zip(names, tail_refs)), base=main.chunks * main.rows, start=main.chunks)
    tail.chunks, tail.rows = tail.rxa.shape[0], tail.rxa.shape[2]
    def rows_of(g, c):
        return pl.ds(pl.multiple_of(g.base + c * g.rows, 8), g.rows)

    def remote(src, dst, send, recv, **where):
        return pltpu.make_async_remote_copy(
            src_ref=src, dst_ref=dst, send_sem=send, recv_sem=recv, device_id=where, device_id_type=MESH
        )

    def far_x(g, c):
        return remote(grad.at[at_d, rows_of(g, c), left], g.rxa.at[c, 1], g.p1_send.at[c, 0], g.p1_recv.at[c, 0], dp=at_x)

    def far_y(g, c):
        return remote(grad.at[at_d, rows_of(g, c), right], g.rxb.at[c, 1], g.p1_send.at[c, 1], g.p1_recv.at[c, 1], dp=at_y)

    def near_x(g, c):
        return remote(grad.at[at_x, rows_of(g, c), left], g.rxa.at[c, 0], g.p1_send.at[c, 2], g.p1_recv.at[c, 2], dp=at_x)

    def near_y(g, c):
        return remote(grad.at[at_y, rows_of(g, c), right], g.rxb.at[c, 0], g.p1_send.at[c, 3], g.p1_recv.at[c, 3], dp=at_y)

    def sum_y(g, c):
        return remote(g.txa.at[c], g.r2a.at[c], g.p2_send.at[c, 0], g.p2_recv.at[c, 0], dp=at_y)

    def unit_y(g, c):
        return remote(g.tsa.at[c], g.rsa.at[c], g.p2_send.at[c, 1], g.p2_recv.at[c, 1], dp=at_y)

    def sum_x(g, c):
        return remote(g.txb.at[c], g.r2b.at[c], g.p2_send.at[c, 2], g.p2_recv.at[c, 2], dp=at_x)

    def unit_x(g, c):
        return remote(g.tsb.at[c], g.rsb.at[c], g.p2_send.at[c, 3], g.p2_recv.at[c, 3], dp=at_x)

    def publish(g, c, hop):
        return remote(
            g.zs.at[c, hop - 1], g.zr.at[eng, hop, c], g.z_send.at[c, hop], g.z_recv.at[c, hop], tp=(tp + hop) % ranks
        )

    def forward(g, c, hop):
        block = g.zr.at[eng, hop, c]
        return remote(block, block, g.f_send.at[c, hop], g.f_recv.at[c, hop], eng=1 - eng)

    def arrival(g, c, hop):
        block = g.zr.at[1 - eng, hop, c]
        return remote(block, block, g.f_send.at[c, hop], g.f_recv.at[c, hop], eng=1 - eng)

    def load_own(g, c):
        return [pltpu.make_async_copy(grad.at[me, rows_of(g, c)], g.own.at[c % 2], g.own_sem.at[c % 2])]

    def load_side(g, c):
        rows = rows_of(g, c)
        return [
            pltpu.make_async_copy(grad.at[at_y, rows, left], g.side_a.at[c % 2], g.side_sem.at[c % 2, 0]),
            pltpu.make_async_copy(grad.at[at_x, rows, right], g.side_b.at[c % 2], g.side_sem.at[c % 2, 1]),
        ]

    def load_old(g, c):
        return [
            pltpu.make_async_copy(states[i].at[rows_of(g, c)], g.old.at[c % 2, i], g.old_sem.at[c % 2, i])
            for i in range(3)
        ]

    def start(copies):
        for copy in copies:
            copy.start()

    def wait(copies):
        for copy in copies:
            copy.wait()

    pl.semaphore_wait(barrier, 2 + ranks)
    for c in range(FAR):
        start([far_x(main, c), far_y(main, c)])
        if c < NEAR:
            start([near_x(main, c), near_y(main, c)])
    for c in range(2):
        start(load_side(main, c) + load_own(main, c) + load_old(main, c))
    for c in range(tail.chunks):
        start(load_side(tail, c) + load_own(tail, c) + load_old(tail, c))

    count = jnp.full((1, 128), adam_step[0], jnp.int32).astype(jnp.float32)
    scale_one = 1.0 / (1.0 - jnp.exp(count * math.log(beta_one)))
    scale_two = 1.0 / (1.0 - jnp.exp(count * math.log(beta_two)))

    def reduce_side(g, c):
        slot = c % 2
        wait(load_side(g, c))
        far_x(g, c).wait_recv()
        pack_sum(g.side_a.at[slot], g.rxa.at[c, 1], g.txa.at[c], g.tsa.at[c])
        start([sum_y(g, c), unit_y(g, c)])
        far_y(g, c).wait_recv()
        pack_sum(g.side_b.at[slot], g.rxb.at[c, 1], g.txb.at[c], g.tsb.at[c])
        start([sum_x(g, c), unit_x(g, c)])

        @pl.when(c + 2 < g.chunks)
        def _():
            start(load_side(g, c + 2))

    def update(g, c):
        slot, rows = c % 2, rows_of(g, c)
        wait(load_own(g, c) + load_old(g, c))
        for copy in (near_x, near_y, sum_y, unit_y, sum_x, unit_x):
            copy(g, c).wait_recv()

        def spread_out(value):
            return stacked(jnp.broadcast_to(value, (g.rows, 128)), STRIP // 128, 1)

        one, two = spread_out(scale_one), spread_out(scale_two)
        unit_a, unit_b = spread_out(g.rsa[c]), spread_out(g.rsb[c])
        for strip in range(columns // STRIP):
            at = pl.ds(strip * STRIP, STRIP)
            side = strip * STRIP // half
            inner = pl.ds(strip * STRIP - side * half, STRIP)
            got, sums, unit = ((g.rxa, g.r2a, unit_a), (g.rxb, g.r2b, unit_b))[side]
            summed = g.own[slot, :, at].astype(jnp.float32) + got[c, 0, :, inner].astype(jnp.float32)
            summed += sums[c, :, inner].astype(jnp.int32).astype(jnp.float32) * unit
            first_now = beta_one * g.old[slot, 1, :, at] + (1.0 - beta_one) * summed
            second_now = beta_two * g.old[slot, 2, :, at] + (1.0 - beta_two) * summed * summed
            was = g.old[slot, 0, :, at]
            step = (first_now * one) / (jnp.sqrt(second_now * two) + eps_value)
            now = was - rate_value * (step + decay_value * was)
            new_master[rows, at] = now
            new_first[rows, at] = first_now
            new_second[rows, at] = second_now
            block = strip * STRIP // width
            g.held[block, :, pl.ds(strip * STRIP - block * width, STRIP)] = now.astype(jnp.bfloat16)
        for hop in range(1, ranks):
            g.zs[c, hop - 1] = g.held[rank_map[(tp + hop) % ranks]]
            publish(g, c, hop).start()
        g.zr[eng, 0, c] = g.held[rank_map[tp]]
        forward(g, c, 0).start()

        @pl.when(c + 2 < g.chunks)
        def _():
            start(load_own(g, c + 2) + load_old(g, c + 2))

    def spread(g, c):
        for hop in range(1, ranks):
            publish(g, c, hop).wait_recv()
            forward(g, c, hop).start()

    def merge(g, c):
        for hop in range(ranks):
            arrival(g, c, hop).wait_recv()
            for part in range(2):
                rollout[(tp + ranks - hop) % ranks, rows_of(g, c), part, :] = g.zr[part, hop, c]

    def at_step(s, lag, act):
        for g in (main, tail):
            c = s - lag - g.start

            @pl.when((c >= 0) & (c < g.chunks))
            def _():
                act(g, c)

    def send_far(g, c):
        start([far_x(g, c), far_y(g, c)])

    def send_near(g, c):
        start([near_x(g, c), near_y(g, c)])

    def drain(g, c):
        for copy in (far_x, far_y, near_x, near_y, sum_y, unit_y, sum_x, unit_x):
            copy(g, c).wait_send()
        for hop in range(ranks):
            forward(g, c, hop).wait_send()
            if hop:
                publish(g, c, hop).wait_send()

    def body(s, carry):
        at_step(s, 0, reduce_side)
        at_step(s, -FAR, send_far)
        at_step(s, -NEAR, send_near)
        at_step(s, UPDATE, update)
        at_step(s, SPREAD, spread)
        at_step(s, MERGE, merge)
        at_step(s, MERGE + 1, drain)
        return carry

    lax.fori_loop(0, main.chunks + tail.chunks + MERGE + 1, body, 0)


def flush(*refs):
    count = (len(refs) - 1) // 2
    copies = [pltpu.make_async_copy(refs[i], refs[count + i], refs[-1].at[i]) for i in range(count)]
    for copy in copies:
        copy.start()
    for copy in copies:
        copy.wait()


def shards(grad_parts, master, first_moment, second_moment, adam_step, rank_map):
    replicas, ranks = lax.axis_size("dp"), lax.axis_size("tp")
    row_count, columns = master.shape[1], master.shape[2]
    half, width = columns // 2, columns // ranks
    grad = grad_parts.reshape(replicas, row_count, columns)
    states = [s.reshape(row_count, columns) for s in (master, first_moment, second_moment)]
    smem, anywhere = pl.BlockSpec(memory_space=pltpu.SMEM), pl.BlockSpec(memory_space=pl.ANY)
    vmem, dma = pltpu.VMEM, pltpu.SemaphoreType.DMA
    short, brain, single = jnp.int16, jnp.bfloat16, jnp.float32

    def scratch(chunks, rows):
        shapes = {name: vmem((chunks, 2, rows, half), brain) for name in ("rxa", "rxb")}
        shapes |= {name: vmem((chunks, rows, half), short) for name in ("txa", "txb", "r2a", "r2b")}
        shapes |= {name: vmem((chunks, 1, 128), single) for name in ("tsa", "tsb", "rsa", "rsb")}
        shapes["zs"] = vmem((chunks, ranks - 1, rows, width), brain)
        shapes["zr"] = vmem((2, ranks, chunks, rows, width), brain)
        shapes["own"] = vmem((2, rows, columns), brain)
        shapes |= {name: vmem((2, rows, half), brain) for name in ("side_a", "side_b")}
        shapes["old"] = vmem((2, 3, rows, columns), single)
        shapes["held"] = vmem((ranks, rows, width), brain)
        shapes |= {name: dma((chunks, 4)) for name in ("p1_send", "p1_recv", "p2_send", "p2_recv")}
        shapes |= {name: dma((chunks, ranks)) for name in ("z_send", "z_recv", "f_send", "f_recv")}
        shapes |= {"own_sem": dma((2,)), "side_sem": dma((2, 2)), "old_sem": dma((2, 3))}
        return shapes

    main = scratch(row_count // ROWS - 1, ROWS)
    tail = scratch(ROWS // TAIL, TAIL)
    results = pl.pallas_call(
        functools.partial(kernel, ranks, tuple(main)),
        out_shape=[vmem(s.shape, s.dtype) for s in states] + [vmem((ranks, row_count, 2, width), brain)],
        in_specs=[smem, smem] + [anywhere] * 4,
        out_specs=[pl.BlockSpec(memory_space=pltpu.VMEM)] * 4,
        scratch_shapes=[*main.values(), *tail.values()],
        compiler_params=pltpu.CompilerParams(
            collective_id=0, has_side_effects=True, vmem_limit_bytes=34 * 1024 * 1024
        ),
        name="exchange",
    )(rank_map, adam_step, grad, *states)
    *outs, rollout = pl.pallas_call(
        flush,
        out_shape=[jax.ShapeDtypeStruct(r.shape, r.dtype) for r in results],
        in_specs=[anywhere] * 4,
        out_specs=[anywhere] * 4,
        scratch_shapes=[dma((4,))],
        compiler_params=pltpu.CompilerParams(vmem_limit_bytes=1024 * 1024),
        name="flush",
    )(*results)
    return (*(o.reshape(master.shape) for o in outs), rollout.reshape(ranks, row_count, 2, 1, width))


def solution(mesh):
    sizes = dict(mesh.shape)

    def step(grad_parts, master, *rest):
        columns = master.shape[2] // sizes["eng"]
        width = columns // sizes["tp"]
        rows = master.shape[1] // sizes["dp"]
        fits = sizes["dp"] == 4 and sizes["eng"] == 2 and width % STRIP == 0 and (columns // 2) % STRIP == 0
        fits = fits and rows % ROWS == 0 and rows // ROWS > FAR + 1
        return jax.shard_map(
            shards if fits else plain_shards,
            mesh=mesh,
            in_specs=(
                P("dp", "tp", None, "eng"),
                P("tp", "dp", "eng"),
                P("tp", "dp", "eng"),
                P("tp", "dp", "eng"),
                P(),
                P(),
            ),
            out_specs=(
                P("tp", "dp", "eng"),
                P("tp", "dp", "eng"),
                P("tp", "dp", "eng"),
                P(None, "dp", None, "tp", None),
            ),
            check_vma=False,
        )(grad_parts, master, *rest)

    return step
```

```python
import functools
import math
import types
import jax
import jax.numpy as jnp
from jax import lax
from jax.experimental import pallas as pl
from jax.experimental.pallas import tpu as pltpu
from jax.sharding import PartitionSpec as P

beta_one = 0.9
beta_two = 0.95
rate_value = 0.001
decay_value = 0.01
eps_value = 1e-08

ROWS = 16
TAIL = 8
FAR, NEAR = 2, 1
UPDATE, SPREAD, MERGE = 1, 3, 4
STRIP = 256
TOP = 32767.0
TINY = 1e-30
MESH = pl.DeviceIdType.MESH


def corrections(adam_step):
    count = adam_step[0].astype(jnp.float32)
    return 1.0 - jnp.power(beta_one, count), 1.0 - jnp.power(beta_two, count)


def plain_shards(grad_parts, master, first_moment, second_moment, adam_step, rank_map):
    summed = lax.psum_scatter(grad_parts.astype(jnp.float32), "dp", scatter_dimension=2, tiled=True)
    summed = summed.reshape(master.shape)
    fix_one, fix_two = corrections(adam_step)
    new_first = beta_one * first_moment + (1.0 - beta_one) * summed
    new_second = beta_two * second_moment + (1.0 - beta_two) * summed * summed
    first_hat = new_first / fix_one
    second_hat = new_second / fix_two
    new_master = master - rate_value * (
        first_hat / (jnp.sqrt(second_hat) + eps_value) + decay_value * master
    )
    row_count = master.shape[1]
    ranks = lax.axis_size("tp")
    block_width = master.shape[2] // ranks
    piece = new_master.astype(jnp.bfloat16).reshape(1, row_count, 1, ranks, block_width)
    ordered = jnp.take(piece, rank_map, axis=3)
    placed = lax.all_to_all(ordered, "tp", split_axis=3, concat_axis=0, tiled=True)
    rollout = lax.all_gather(placed, "eng", axis=2, tiled=True)
    return (new_master, new_first, new_second, rollout)


def stacked(value, times, axis):
    return jnp.concatenate([value] * times, axis=axis) if times > 1 else value


def pack_sum(near, far, packed, scale):
    rows, tiles = packed.shape[0], packed.shape[1] // 128
    tops = [jnp.zeros((8, 128), jnp.float32) for _ in range(4)]
    for tile in range(tiles):
        columns = pl.ds(tile * 128, 128)
        size = jnp.abs(near[:, columns].astype(jnp.float32) + far[:, columns].astype(jnp.float32))
        for part in range(rows // 8):
            slot = (2 * tile + part) % 4
            tops[slot] = jnp.maximum(tops[slot], size[8 * part : 8 * part + 8])
    top = jnp.maximum(jnp.maximum(tops[0], tops[1]), jnp.maximum(tops[2], tops[3]))
    top = jnp.maximum(jnp.max(top, axis=0, keepdims=True), TINY)
    scale[...] = top * (1.0 / TOP)
    factor = jnp.broadcast_to(TOP / top, (rows, 128))
    for tile in range(tiles):
        columns = pl.ds(tile * 128, 128)
        value = near[:, columns].astype(jnp.float32) + far[:, columns].astype(jnp.float32)
        packed[:, columns] = jnp.round(value * factor).astype(jnp.int32).astype(jnp.int16)


def kernel(ranks, names, rank_map, adam_step, grad, master, first, second, *refs):
    new_master, new_first, new_second, rollout = refs[:4]
    body_refs, tail_refs = refs[4 : 4 + len(names)], refs[4 + len(names) :]
    columns = grad.shape[2]
    half = columns // 2
    width = columns // ranks
    me, tp, eng = (lax.axis_index(a) for a in ("dp", "tp", "eng"))
    at_x = me + 1 - 2 * (me % 2)
    at_y = (me + 2) % 4
    at_d = 3 - me
    barrier = pltpu.get_barrier_semaphore()
    for where in (
        [{"dp": at_x}, {"dp": at_y}, {"eng": 1 - eng}] + [{"tp": (tp + hop) % ranks} for hop in range(1, ranks)]
    ):
        pl.semaphore_signal(barrier, inc=1, device_id=where, device_id_type=MESH)
    left, right = pl.ds(0, half), pl.ds(half, half)
    states = (master, first, second)
    main = types.SimpleNamespace(**dict(zip(names, body_refs)), base=0, start=0)
    main.chunks, main.rows = main.rxa.shape[0], main.rxa.shape[2]
    tail = types.SimpleNamespace(**dict(zip(names, tail_refs)), base=main.chunks * main.rows, start=main.chunks)
    tail.chunks, tail.rows = tail.rxa.shape[0], tail.rxa.shape[2]
    def rows_of(g, c):
        return pl.ds(pl.multiple_of(g.base + c * g.rows, 8), g.rows)

    def remote(src, dst, send, recv, **where):
        return pltpu.make_async_remote_copy(
            src_ref=src, dst_ref=dst, send_sem=send, recv_sem=recv, device_id=where, device_id_type=MESH
        )

    def far_x(g, c):
        return remote(grad.at[at_d, rows_of(g, c), left], g.rxa.at[c, 1], g.sent.at[0], g.far_sem.at[c], dp=at_x)

    def far_y(g, c):
        return remote(grad.at[at_d, rows_of(g, c), right], g.rxb.at[c, 1], g.sent.at[1], g.far_sem.at[c], dp=at_y)

    def near_x(g, c):
        return remote(grad.at[at_x, rows_of(g, c), left], g.rxa.at[c, 0], g.sent.at[0], g.mid_sem.at[c], dp=at_x)

    def near_y(g, c):
        return remote(grad.at[at_y, rows_of(g, c), right], g.rxb.at[c, 0], g.sent.at[1], g.mid_sem.at[c], dp=at_y)

    def sum_y(g, c):
        return remote(g.txa.at[c], g.r2a.at[c], g.sent.at[2], g.mid_sem.at[c], dp=at_y)

    def sum_x(g, c):
        return remote(g.txb.at[c], g.r2b.at[c], g.sent.at[2], g.mid_sem.at[c], dp=at_x)

    def unit_y(g, c):
        return remote(g.ts.at[c, 0], g.rs.at[c, 0], g.sent.at[3], g.unit_sem.at[c], dp=at_y)

    def unit_x(g, c):
        return remote(g.ts.at[c, 1], g.rs.at[c, 1], g.sent.at[3], g.unit_sem.at[c], dp=at_x)

    def publish(g, c, hop):
        return remote(g.zs.at[c, hop - 1], g.zr.at[eng, hop, c], g.sent.at[4], g.z_sem.at[c], tp=(tp + hop) % ranks)

    def forward(g, c, hop):
        block = g.zr.at[eng, hop, c]
        return remote(block, block, g.sent.at[5], g.f_sem.at[c], eng=1 - eng)

    def wait_bytes(like, sem):
        pltpu.make_async_copy(like, like, sem).wait()

    def load_own(g, c):
        return [pltpu.make_async_copy(grad.at[me, rows_of(g, c)], g.own.at[c % 2], g.own_sem.at[c % 2])]

    def load_side(g, c):
        rows = rows_of(g, c)
        return [
            pltpu.make_async_copy(grad.at[at_y, rows, left], g.side_a.at[c % 2], g.side_sem.at[c % 2, 0]),
            pltpu.make_async_copy(grad.at[at_x, rows, right], g.side_b.at[c % 2], g.side_sem.at[c % 2, 1]),
        ]

    def load_old(g, c):
        return [
            pltpu.make_async_copy(states[i].at[rows_of(g, c)], g.old.at[c % 2, i], g.old_sem.at[c % 2, i])
            for i in range(3)
        ]

    def start(copies):
        for copy in copies:
            copy.start()

    def wait(copies):
        for copy in copies:
            copy.wait()

    pl.semaphore_wait(barrier, 2 + ranks)
    for c in range(FAR):
        start([far_x(main, c), far_y(main, c)])
        if c < NEAR:
            start([near_x(main, c), near_y(main, c)])
    for c in range(2):
        start(load_side(main, c) + load_own(main, c) + load_old(main, c))
    for c in range(tail.chunks):
        start(load_side(tail, c) + load_own(tail, c) + load_old(tail, c))

    count = jnp.full((1, 128), adam_step[0], jnp.int32).astype(jnp.float32)
    scale_one = 1.0 / (1.0 - jnp.exp(count * math.log(beta_one)))
    scale_two = 1.0 / (1.0 - jnp.exp(count * math.log(beta_two)))

    def reduce_side(g, c):
        slot = c % 2
        wait(load_side(g, c))
        wait_bytes(g.rxa.at[c], g.far_sem.at[c])
        pack_sum(g.side_a.at[slot], g.rxa.at[c, 1], g.txa.at[c], g.ts.at[c, 0])
        start([sum_y(g, c), unit_y(g, c)])
        pack_sum(g.side_b.at[slot], g.rxb.at[c, 1], g.txb.at[c], g.ts.at[c, 1])
        start([sum_x(g, c), unit_x(g, c)])

        @pl.when(c + 2 < g.chunks)
        def _():
            start(load_side(g, c + 2))

    def update(g, c):
        slot, rows = c % 2, rows_of(g, c)
        wait(load_own(g, c) + load_old(g, c))
        wait_bytes(g.own, g.mid_sem.at[c])
        wait_bytes(g.rs.at[c], g.unit_sem.at[c])

        def spread_out(value):
            return stacked(jnp.broadcast_to(value, (g.rows, 128)), STRIP // 128, 1)

        one, two = spread_out(scale_one), spread_out(scale_two)
        unit_a, unit_b = spread_out(g.rs[c, 0]), spread_out(g.rs[c, 1])
        for strip in range(columns // STRIP):
            at = pl.ds(strip * STRIP, STRIP)
            side = strip * STRIP // half
            inner = pl.ds(strip * STRIP - side * half, STRIP)
            got, sums, unit = ((g.rxa, g.r2a, unit_a), (g.rxb, g.r2b, unit_b))[side]
            summed = g.own[slot, :, at].astype(jnp.float32) + got[c, 0, :, inner].astype(jnp.float32)
            summed += sums[c, :, inner].astype(jnp.int32).astype(jnp.float32) * unit
            first_now = beta_one * g.old[slot, 1, :, at] + (1.0 - beta_one) * summed
            second_now = beta_two * g.old[slot, 2, :, at] + (1.0 - beta_two) * summed * summed
            was = g.old[slot, 0, :, at]
            step = (first_now * one) / (jnp.sqrt(second_now * two) + eps_value)
            now = was - rate_value * (step + decay_value * was)
            new_master[rows, at] = now
            new_first[rows, at] = first_now
            new_second[rows, at] = second_now
            block = strip * STRIP // width
            g.held[block, :, pl.ds(strip * STRIP - block * width, STRIP)] = now.astype(jnp.bfloat16)
        for hop in range(1, ranks):
            g.zs[c, hop - 1] = g.held[rank_map[(tp + hop) % ranks]]
            publish(g, c, hop).start()
        g.zr[eng, 0, c] = g.held[rank_map[tp]]
        forward(g, c, 0).start()

        @pl.when(c + 2 < g.chunks)
        def _():
            start(load_own(g, c + 2) + load_old(g, c + 2))

    def spread(g, c):
        wait_bytes(g.zs.at[c], g.z_sem.at[c])
        for hop in range(1, ranks):
            forward(g, c, hop).start()

    def merge(g, c):
        wait_bytes(g.zr.at[1 - eng, :, c], g.f_sem.at[c])
        for hop in range(ranks):
            for part in range(2):
                rollout[(tp + ranks - hop) % ranks, rows_of(g, c), part, :] = g.zr[part, hop, c]

    def at_step(s, lag, act):
        for g in (main, tail):
            c = s - lag - g.start

            @pl.when((c >= 0) & (c < g.chunks))
            def _():
                act(g, c)

    def send_far(g, c):
        start([far_x(g, c), far_y(g, c)])

    def send_near(g, c):
        start([near_x(g, c), near_y(g, c)])

    def body(s, carry):
        at_step(s, 0, reduce_side)
        at_step(s, -FAR, send_far)
        at_step(s, -NEAR, send_near)
        at_step(s, UPDATE, update)
        at_step(s, SPREAD, spread)
        at_step(s, MERGE, merge)
        return carry

    lax.fori_loop(0, main.chunks + tail.chunks + MERGE, body, 0)
    for g in (main, tail):
        for i, like in enumerate((g.rxa, g.rxb, g.rxa, g.ts, g.zs, g.zr.at[eng])):
            wait_bytes(like, g.sent.at[i])


def flush(*refs):
    count = (len(refs) - 1) // 2
    copies = [pltpu.make_async_copy(refs[i], refs[count + i], refs[-1].at[i]) for i in range(count)]
    for copy in copies:
        copy.start()
    for copy in copies:
        copy.wait()


def shards(grad_parts, master, first_moment, second_moment, adam_step, rank_map):
    replicas, ranks = lax.axis_size("dp"), lax.axis_size("tp")
    row_count, columns = master.shape[1], master.shape[2]
    half, width = columns // 2, columns // ranks
    grad = grad_parts.reshape(replicas, row_count, columns)
    states = [s.reshape(row_count, columns) for s in (master, first_moment, second_moment)]
    smem, anywhere = pl.BlockSpec(memory_space=pltpu.SMEM), pl.BlockSpec(memory_space=pl.ANY)
    vmem, dma = pltpu.VMEM, pltpu.SemaphoreType.DMA
    short, brain, single = jnp.int16, jnp.bfloat16, jnp.float32

    def scratch(chunks, rows):
        shapes = {name: vmem((chunks, 2, rows, half), brain) for name in ("rxa", "rxb")}
        shapes |= {name: vmem((chunks, rows, half), short) for name in ("txa", "txb", "r2a", "r2b")}
        shapes |= {name: vmem((chunks, 2, 1, 128), single) for name in ("ts", "rs")}
        shapes["zs"] = vmem((chunks, ranks - 1, rows, width), brain)
        shapes["zr"] = vmem((2, ranks, chunks, rows, width), brain)
        shapes["own"] = vmem((2, rows, columns), brain)
        shapes |= {name: vmem((2, rows, half), brain) for name in ("side_a", "side_b")}
        shapes["old"] = vmem((2, 3, rows, columns), single)
        shapes["held"] = vmem((ranks, rows, width), brain)
        shapes |= {name: dma((chunks,)) for name in ("far_sem", "mid_sem", "unit_sem", "z_sem", "f_sem")}
        shapes["sent"] = dma((6,))
        shapes |= {"own_sem": dma((2,)), "side_sem": dma((2, 2)), "old_sem": dma((2, 3))}
        return shapes

    main = scratch(row_count // ROWS - 1, ROWS)
    tail = scratch(ROWS // TAIL, TAIL)
    results = pl.pallas_call(
        functools.partial(kernel, ranks, tuple(main)),
        out_shape=[vmem(s.shape, s.dtype) for s in states] + [vmem((ranks, row_count, 2, width), brain)],
        in_specs=[smem, smem] + [anywhere] * 4,
        out_specs=[pl.BlockSpec(memory_space=pltpu.VMEM)] * 4,
        scratch_shapes=[*main.values(), *tail.values()],
        compiler_params=pltpu.CompilerParams(
            collective_id=0, has_side_effects=True, vmem_limit_bytes=34 * 1024 * 1024
        ),
        name="exchange",
    )(rank_map, adam_step, grad, *states)
    *outs, rollout = pl.pallas_call(
        flush,
        out_shape=[jax.ShapeDtypeStruct(r.shape, r.dtype) for r in results],
        in_specs=[anywhere] * 4,
        out_specs=[anywhere] * 4,
        scratch_shapes=[dma((4,))],
        compiler_params=pltpu.CompilerParams(vmem_limit_bytes=1024 * 1024),
        name="flush",
    )(*results)
    return (*(o.reshape(master.shape) for o in outs), rollout.reshape(ranks, row_count, 2, 1, width))


def solution(mesh):
    sizes = dict(mesh.shape)

    def step(grad_parts, master, *rest):
        columns = master.shape[2] // sizes["eng"]
        width = columns // sizes["tp"]
        rows = master.shape[1] // sizes["dp"]
        fits = sizes["dp"] == 4 and sizes["eng"] == 2 and width % STRIP == 0 and (columns // 2) % STRIP == 0
        fits = fits and rows % ROWS == 0 and rows // ROWS > FAR + 1
        return jax.shard_map(
            shards if fits else plain_shards,
            mesh=mesh,
            in_specs=(
                P("dp", "tp", None, "eng"),
                P("tp", "dp", "eng"),
                P("tp", "dp", "eng"),
                P("tp", "dp", "eng"),
                P(),
                P(),
            ),
            out_specs=(
                P("tp", "dp", "eng"),
                P("tp", "dp", "eng"),
                P("tp", "dp", "eng"),
                P(None, "dp", None, "tp", None),
            ),
            check_vma=False,
        )(grad_parts, master, *rest)

    return step
```

```python
import functools
import math
import types
import jax
import jax.numpy as jnp
from jax import lax
from jax.experimental import pallas as pl
from jax.experimental.pallas import tpu as pltpu
from jax.sharding import PartitionSpec as P

beta_one = 0.9
beta_two = 0.95
rate_value = 0.001
decay_value = 0.01
eps_value = 1e-08

ROWS = 16
TAIL = 8
FAR, NEAR = 2, 1
RING = 8
UPDATE, SPREAD, MERGE = 1, 3, 4
STRIP = 256
TOP = 32767.0
TINY = 1e-30
MESH = pl.DeviceIdType.MESH


def corrections(adam_step):
    count = adam_step[0].astype(jnp.float32)
    return 1.0 - jnp.power(beta_one, count), 1.0 - jnp.power(beta_two, count)


def plain_shards(grad_parts, master, first_moment, second_moment, adam_step, rank_map):
    summed = lax.psum_scatter(grad_parts.astype(jnp.float32), "dp", scatter_dimension=2, tiled=True)
    summed = summed.reshape(master.shape)
    fix_one, fix_two = corrections(adam_step)
    new_first = beta_one * first_moment + (1.0 - beta_one) * summed
    new_second = beta_two * second_moment + (1.0 - beta_two) * summed * summed
    first_hat = new_first / fix_one
    second_hat = new_second / fix_two
    new_master = master - rate_value * (
        first_hat / (jnp.sqrt(second_hat) + eps_value) + decay_value * master
    )
    row_count = master.shape[1]
    ranks = lax.axis_size("tp")
    block_width = master.shape[2] // ranks
    piece = new_master.astype(jnp.bfloat16).reshape(1, row_count, 1, ranks, block_width)
    ordered = jnp.take(piece, rank_map, axis=3)
    placed = lax.all_to_all(ordered, "tp", split_axis=3, concat_axis=0, tiled=True)
    rollout = lax.all_gather(placed, "eng", axis=2, tiled=True)
    return (new_master, new_first, new_second, rollout)


def stacked(value, times, axis):
    return jnp.concatenate([value] * times, axis=axis) if times > 1 else value


def pack_sum(near, far, packed, scale):
    rows, tiles = packed.shape[0], packed.shape[1] // 128
    tops = [jnp.zeros((8, 128), jnp.float32) for _ in range(4)]
    for tile in range(tiles):
        columns = pl.ds(tile * 128, 128)
        size = jnp.abs(near[:, columns].astype(jnp.float32) + far[:, columns].astype(jnp.float32))
        for part in range(rows // 8):
            slot = (2 * tile + part) % 4
            tops[slot] = jnp.maximum(tops[slot], size[8 * part : 8 * part + 8])
    top = jnp.maximum(jnp.maximum(tops[0], tops[1]), jnp.maximum(tops[2], tops[3]))
    top = jnp.maximum(jnp.max(top, axis=0, keepdims=True), TINY)
    scale[...] = top * (1.0 / TOP)
    factor = jnp.broadcast_to(TOP / top, (rows, 128))
    for tile in range(tiles):
        columns = pl.ds(tile * 128, 128)
        value = near[:, columns].astype(jnp.float32) + far[:, columns].astype(jnp.float32)
        packed[:, columns] = jnp.round(value * factor).astype(jnp.int32).astype(jnp.int16)


def kernel(ranks, names, rank_map_in, adam_step_in, grad, master, first, second, *refs):
    new_master, new_first, new_second, rollout, rank_map, adam_step, small_sem = refs[:7]
    body_refs, tail_refs = refs[7 : 7 + len(names)], refs[7 + len(names) :]
    columns = grad.shape[2]
    half = columns // 2
    width = columns // ranks
    me, tp, eng = (lax.axis_index(a) for a in ("dp", "tp", "eng"))
    at_x = me + 1 - 2 * (me % 2)
    at_y = (me + 2) % 4
    at_d = 3 - me
    barrier = pltpu.get_barrier_semaphore()
    for where in (
        [{"dp": at_x}, {"dp": at_y}, {"eng": 1 - eng}] + [{"tp": (tp + hop) % ranks} for hop in range(1, ranks)]
    ):
        pl.semaphore_signal(barrier, inc=1, device_id=where, device_id_type=MESH)
    left, right = pl.ds(0, half), pl.ds(half, half)
    states = (master, first, second)
    main = types.SimpleNamespace(**dict(zip(names, body_refs)), base=0, start=0)
    main.chunks, main.rows = main.rxa.shape[0], main.rxa.shape[2]
    tail = types.SimpleNamespace(**dict(zip(names, tail_refs)), base=main.chunks * main.rows, start=main.chunks)
    tail.chunks, tail.rows = tail.rxa.shape[0], tail.rxa.shape[2]
    def rows_of(g, c):
        return pl.ds(pl.multiple_of(g.base + c * g.rows, 8), g.rows)

    def remote(src, dst, send, recv, **where):
        return pltpu.make_async_remote_copy(
            src_ref=src, dst_ref=dst, send_sem=send, recv_sem=recv, device_id=where, device_id_type=MESH
        )

    def far_x(g, c):
        return remote(grad.at[at_d, rows_of(g, c), left], g.rxa.at[c, 1], g.sent.at[0], g.far_sem.at[c % RING], dp=at_x)

    def far_y(g, c):
        return remote(grad.at[at_d, rows_of(g, c), right], g.rxb.at[c, 1], g.sent.at[1], g.far_sem.at[c % RING], dp=at_y)

    def near_x(g, c):
        return remote(grad.at[at_x, rows_of(g, c), left], g.rxa.at[c, 0], g.sent.at[0], g.mid_sem.at[c % RING], dp=at_x)

    def near_y(g, c):
        return remote(grad.at[at_y, rows_of(g, c), right], g.rxb.at[c, 0], g.sent.at[1], g.mid_sem.at[c % RING], dp=at_y)

    def sum_y(g, c):
        return remote(g.txa.at[c], g.r2a.at[c], g.sent.at[2], g.mid_sem.at[c % RING], dp=at_y)

    def sum_x(g, c):
        return remote(g.txb.at[c], g.r2b.at[c], g.sent.at[2], g.mid_sem.at[c % RING], dp=at_x)

    def unit_y(g, c):
        return remote(g.ts.at[c, 0], g.rs.at[c, 0], g.sent.at[3], g.unit_sem.at[c % RING], dp=at_y)

    def unit_x(g, c):
        return remote(g.ts.at[c, 1], g.rs.at[c, 1], g.sent.at[3], g.unit_sem.at[c % RING], dp=at_x)

    def publish(g, c, hop):
        return remote(g.zs.at[c, hop - 1], g.zr.at[eng, hop, c], g.sent.at[4], g.z_sem.at[c % RING], tp=(tp + hop) % ranks)

    def forward(g, c, hop):
        block = g.zr.at[eng, hop, c]
        return remote(block, block, g.sent.at[5], g.f_sem.at[c % RING], eng=1 - eng)

    def wait_bytes(like, sem):
        pltpu.make_async_copy(like, like, sem).wait()

    def load_side(g, c):
        rows, sem = rows_of(g, c), g.load_sem.at[0, c % 2]
        return [
            pltpu.make_async_copy(grad.at[at_y, rows, left], g.side.at[c % 2, 0], sem),
            pltpu.make_async_copy(grad.at[at_x, rows, right], g.side.at[c % 2, 1], sem),
        ]

    def load_own(g, c):
        return [pltpu.make_async_copy(grad.at[me, rows_of(g, c)], g.own.at[c % 2], g.load_sem.at[1, c % 2])]

    def load_old(g, c):
        sem = g.load_sem.at[2, c % 2]
        return [pltpu.make_async_copy(states[i].at[rows_of(g, c)], g.old.at[c % 2, i], sem) for i in range(3)]

    def start(copies):
        for copy in copies:
            copy.start()

    pl.semaphore_wait(barrier, 2 + ranks)
    for c in range(FAR):
        start([far_x(main, c), far_y(main, c)])
        if c < NEAR:
            start([near_x(main, c), near_y(main, c)])
    for c in range(2):
        start(load_side(main, c) + load_own(main, c) + load_old(main, c))
    for c in range(tail.chunks):
        start(load_side(tail, c) + load_own(tail, c) + load_old(tail, c))

    small = [
        pltpu.make_async_copy(rank_map_in, rank_map, small_sem.at[0]),
        pltpu.make_async_copy(adam_step_in, adam_step, small_sem.at[1]),
    ]
    start(small)
    for copy in small:
        copy.wait()
    count = jnp.full((1, 128), adam_step[0], jnp.int32).astype(jnp.float32)
    scale_one = 1.0 / (1.0 - jnp.exp(count * math.log(beta_one)))
    scale_two = 1.0 / (1.0 - jnp.exp(count * math.log(beta_two)))

    def reduce_side(g, c):
        slot = c % 2
        wait_bytes(g.side.at[slot], g.load_sem.at[0, slot])
        wait_bytes(g.rxa.at[c], g.far_sem.at[c % RING])
        pack_sum(g.side.at[slot, 0], g.rxa.at[c, 1], g.txa.at[c], g.ts.at[c, 0])
        start([sum_y(g, c), unit_y(g, c)])
        pack_sum(g.side.at[slot, 1], g.rxb.at[c, 1], g.txb.at[c], g.ts.at[c, 1])
        start([sum_x(g, c), unit_x(g, c)])

        @pl.when(c + 2 < g.chunks)
        def _():
            start(load_side(g, c + 2))

    def update(g, c):
        slot, rows = c % 2, rows_of(g, c)
        wait_bytes(g.own.at[slot], g.load_sem.at[1, slot])
        wait_bytes(g.old.at[slot], g.load_sem.at[2, slot])
        wait_bytes(g.own, g.mid_sem.at[c % RING])
        wait_bytes(g.rs.at[c], g.unit_sem.at[c % RING])

        def spread_out(value):
            return stacked(jnp.broadcast_to(value, (g.rows, 128)), STRIP // 128, 1)

        one, two = spread_out(scale_one), spread_out(scale_two)
        unit_a, unit_b = spread_out(g.rs[c, 0]), spread_out(g.rs[c, 1])
        for strip in range(columns // STRIP):
            at = pl.ds(strip * STRIP, STRIP)
            side = strip * STRIP // half
            inner = pl.ds(strip * STRIP - side * half, STRIP)
            got, sums, unit = ((g.rxa, g.r2a, unit_a), (g.rxb, g.r2b, unit_b))[side]
            summed = g.own[slot, :, at].astype(jnp.float32) + got[c, 0, :, inner].astype(jnp.float32)
            summed += sums[c, :, inner].astype(jnp.int32).astype(jnp.float32) * unit
            first_now = beta_one * g.old[slot, 1, :, at] + (1.0 - beta_one) * summed
            second_now = beta_two * g.old[slot, 2, :, at] + (1.0 - beta_two) * summed * summed
            was = g.old[slot, 0, :, at]
            step = (first_now * one) / (jnp.sqrt(second_now * two) + eps_value)
            now = was - rate_value * (step + decay_value * was)
            new_master[rows, at] = now
            new_first[rows, at] = first_now
            new_second[rows, at] = second_now
            block = strip * STRIP // width
            g.held[block, :, pl.ds(strip * STRIP - block * width, STRIP)] = now.astype(jnp.bfloat16)
        for hop in range(1, ranks):
            g.zs[c, hop - 1] = g.held[rank_map[(tp + hop) % ranks]]
            publish(g, c, hop).start()
        g.zr[eng, 0, c] = g.held[rank_map[tp]]
        forward(g, c, 0).start()

        @pl.when(c + 2 < g.chunks)
        def _():
            start(load_own(g, c + 2) + load_old(g, c + 2))

    def spread(g, c):
        wait_bytes(g.zs.at[c], g.z_sem.at[c % RING])
        for hop in range(1, ranks):
            forward(g, c, hop).start()

    def merge(g, c):
        wait_bytes(g.zr.at[1 - eng, :, c], g.f_sem.at[c % RING])
        for hop in range(ranks):
            for part in range(2):
                rollout[(tp + ranks - hop) % ranks, rows_of(g, c), part, :] = g.zr[part, hop, c]

    def at_step(s, lag, act):
        for g in (main, tail):
            c = s - lag - g.start

            @pl.when((c >= 0) & (c < g.chunks))
            def _():
                act(g, c)

    def send_far(g, c):
        start([far_x(g, c), far_y(g, c)])

    def send_near(g, c):
        start([near_x(g, c), near_y(g, c)])

    def body(s, carry):
        at_step(s, 0, reduce_side)
        at_step(s, -FAR, send_far)
        at_step(s, -NEAR, send_near)
        at_step(s, UPDATE, update)
        at_step(s, SPREAD, spread)
        at_step(s, MERGE, merge)
        return carry

    lax.fori_loop(0, main.chunks + tail.chunks + MERGE, body, 0)
    for g in (main, tail):
        for i, like in enumerate((g.rxa, g.rxb, g.rxa, g.ts, g.zs, g.zr.at[eng])):
            wait_bytes(like, g.sent.at[i])


def flush(*refs):
    count = (len(refs) - 1) // 2
    copies = [pltpu.make_async_copy(refs[i], refs[count + i], refs[-1].at[i]) for i in range(count)]
    for copy in copies:
        copy.start()
    for copy in copies:
        copy.wait()


def shards(grad_parts, master, first_moment, second_moment, adam_step, rank_map):
    replicas, ranks = lax.axis_size("dp"), lax.axis_size("tp")
    row_count, columns = master.shape[1], master.shape[2]
    half, width = columns // 2, columns // ranks
    grad = grad_parts.reshape(replicas, row_count, columns)
    states = [s.reshape(row_count, columns) for s in (master, first_moment, second_moment)]
    anywhere = pl.BlockSpec(memory_space=pl.ANY)
    vmem, dma = pltpu.VMEM, pltpu.SemaphoreType.DMA
    short, brain, single = jnp.int16, jnp.bfloat16, jnp.float32

    def scratch(chunks, rows):
        shapes = {name: vmem((chunks, 2, rows, half), brain) for name in ("rxa", "rxb")}
        shapes |= {name: vmem((chunks, rows, half), short) for name in ("txa", "txb", "r2a", "r2b")}
        shapes |= {name: vmem((chunks, 2, 1, 128), single) for name in ("ts", "rs")}
        shapes["zs"] = vmem((chunks, ranks - 1, rows, width), brain)
        shapes["zr"] = vmem((2, ranks, chunks, rows, width), brain)
        shapes["own"] = vmem((2, rows, columns), brain)
        shapes["side"] = vmem((2, 2, rows, half), brain)
        shapes["old"] = vmem((2, 3, rows, columns), single)
        shapes["held"] = vmem((ranks, rows, width), brain)
        shapes |= {name: dma((min(chunks, RING),)) for name in ("far_sem", "mid_sem", "unit_sem", "z_sem", "f_sem")}
        shapes["sent"] = dma((6,))
        shapes["load_sem"] = dma((3, 2))
        return shapes

    main = scratch(row_count // ROWS - 1, ROWS)
    tail = scratch(ROWS // TAIL, TAIL)
    results = pl.pallas_call(
        functools.partial(kernel, ranks, tuple(main)),
        out_shape=[vmem(s.shape, s.dtype) for s in states] + [vmem((ranks, row_count, 2, width), brain)],
        in_specs=[anywhere] * 6,
        out_specs=[pl.BlockSpec(memory_space=pltpu.VMEM)] * 4,
        scratch_shapes=[
            pltpu.SMEM(rank_map.shape, rank_map.dtype),
            pltpu.SMEM(adam_step.shape, adam_step.dtype),
            dma((2,)),
            *main.values(),
            *tail.values(),
        ],
        compiler_params=pltpu.CompilerParams(
            collective_id=0, has_side_effects=True, vmem_limit_bytes=34 * 1024 * 1024
        ),
        name="exchange",
    )(rank_map, adam_step, grad, *states)
    *outs, rollout = pl.pallas_call(
        flush,
        out_shape=[jax.ShapeDtypeStruct(r.shape, r.dtype) for r in results],
        in_specs=[anywhere] * 4,
        out_specs=[anywhere] * 4,
        scratch_shapes=[dma((4,))],
        compiler_params=pltpu.CompilerParams(vmem_limit_bytes=1024 * 1024),
        name="flush",
    )(*results)
    return (*(o.reshape(master.shape) for o in outs), rollout.reshape(ranks, row_count, 2, 1, width))


def solution(mesh):
    sizes = dict(mesh.shape)

    def step(grad_parts, master, *rest):
        columns = master.shape[2] // sizes["eng"]
        width = columns // sizes["tp"]
        rows = master.shape[1] // sizes["dp"]
        fits = sizes["dp"] == 4 and sizes["eng"] == 2 and width % STRIP == 0 and (columns // 2) % STRIP == 0
        fits = fits and rows % ROWS == 0 and rows // ROWS > FAR + 1
        return jax.shard_map(
            shards if fits else plain_shards,
            mesh=mesh,
            in_specs=(
                P("dp", "tp", None, "eng"),
                P("tp", "dp", "eng"),
                P("tp", "dp", "eng"),
                P("tp", "dp", "eng"),
                P(),
                P(),
            ),
            out_specs=(
                P("tp", "dp", "eng"),
                P("tp", "dp", "eng"),
                P("tp", "dp", "eng"),
                P(None, "dp", None, "tp", None),
            ),
            check_vma=False,
        )(grad_parts, master, *rest)

    return step
```

```python
import functools
import math
import types
import jax
import jax.numpy as jnp
from jax import lax
from jax.experimental import pallas as pl
from jax.experimental.pallas import tpu as pltpu
from jax.sharding import PartitionSpec as P

beta_one = 0.9
beta_two = 0.95
rate_value = 0.001
decay_value = 0.01
eps_value = 1e-08

ROWS = 16
TAIL = 8
FAR, NEAR = 2, 1
RING = 8
UPDATE, SPREAD, MERGE = 1, 4, 5
STRIP = 256
TOP = 32767.0
TINY = 1e-30
MESH = pl.DeviceIdType.MESH


def corrections(adam_step):
    count = adam_step[0].astype(jnp.float32)
    return 1.0 - jnp.power(beta_one, count), 1.0 - jnp.power(beta_two, count)


def plain_shards(grad_parts, master, first_moment, second_moment, adam_step, rank_map):
    summed = lax.psum_scatter(grad_parts.astype(jnp.float32), "dp", scatter_dimension=2, tiled=True)
    summed = summed.reshape(master.shape)
    fix_one, fix_two = corrections(adam_step)
    new_first = beta_one * first_moment + (1.0 - beta_one) * summed
    new_second = beta_two * second_moment + (1.0 - beta_two) * summed * summed
    first_hat = new_first / fix_one
    second_hat = new_second / fix_two
    new_master = master - rate_value * (
        first_hat / (jnp.sqrt(second_hat) + eps_value) + decay_value * master
    )
    row_count = master.shape[1]
    ranks = lax.axis_size("tp")
    block_width = master.shape[2] // ranks
    piece = new_master.astype(jnp.bfloat16).reshape(1, row_count, 1, ranks, block_width)
    ordered = jnp.take(piece, rank_map, axis=3)
    placed = lax.all_to_all(ordered, "tp", split_axis=3, concat_axis=0, tiled=True)
    rollout = lax.all_gather(placed, "eng", axis=2, tiled=True)
    return (new_master, new_first, new_second, rollout)


def stacked(value, times, axis):
    return jnp.concatenate([value] * times, axis=axis) if times > 1 else value


def pack_sum(near, far, packed, scale):
    rows, tiles = packed.shape[0], packed.shape[1] // 128
    tops = [jnp.zeros((8, 128), jnp.float32) for _ in range(4)]
    for tile in range(tiles):
        columns = pl.ds(tile * 128, 128)
        size = jnp.abs(near[:, columns].astype(jnp.float32) + far[:, columns].astype(jnp.float32))
        for part in range(rows // 8):
            slot = (2 * tile + part) % 4
            tops[slot] = jnp.maximum(tops[slot], size[8 * part : 8 * part + 8])
    top = jnp.maximum(jnp.maximum(tops[0], tops[1]), jnp.maximum(tops[2], tops[3]))
    top = jnp.maximum(jnp.max(top, axis=0, keepdims=True), TINY)
    scale[...] = top * (1.0 / TOP)
    factor = jnp.broadcast_to(TOP / top, (rows, 128))
    for tile in range(tiles):
        columns = pl.ds(tile * 128, 128)
        value = near[:, columns].astype(jnp.float32) + far[:, columns].astype(jnp.float32)
        packed[:, columns] = jnp.round(value * factor).astype(jnp.int32).astype(jnp.int16)


def kernel(ranks, names, rank_map_in, adam_step_in, grad, master, first, second, *refs):
    new_master, new_first, new_second, rollout, rank_map, adam_step, small_sem = refs[:7]
    body_refs, tail_refs = refs[7 : 7 + len(names)], refs[7 + len(names) :]
    columns = grad.shape[2]
    half = columns // 2
    width = columns // ranks
    me, tp, eng = (lax.axis_index(a) for a in ("dp", "tp", "eng"))
    at_x = me + 1 - 2 * (me % 2)
    at_y = (me + 2) % 4
    at_d = 3 - me
    barrier = pltpu.get_barrier_semaphore()
    for where in (
        [{"dp": at_x}, {"dp": at_y}, {"eng": 1 - eng}] + [{"tp": (tp + hop) % ranks} for hop in range(1, ranks)]
    ):
        pl.semaphore_signal(barrier, inc=1, device_id=where, device_id_type=MESH)
    left, right = pl.ds(0, half), pl.ds(half, half)
    states = (master, first, second)
    main = types.SimpleNamespace(**dict(zip(names, body_refs)), base=0, start=0)
    main.chunks, main.rows = main.rxa.shape[0], main.rxa.shape[2]
    tail = types.SimpleNamespace(**dict(zip(names, tail_refs)), base=main.chunks * main.rows, start=main.chunks)
    tail.chunks, tail.rows = tail.rxa.shape[0], tail.rxa.shape[2]
    def rows_of(g, c):
        return pl.ds(pl.multiple_of(g.base + c * g.rows, 8), g.rows)

    def remote(src, dst, send, recv, **where):
        return pltpu.make_async_remote_copy(
            src_ref=src, dst_ref=dst, send_sem=send, recv_sem=recv, device_id=where, device_id_type=MESH
        )

    def far_x(g, c):
        return remote(grad.at[at_d, rows_of(g, c), left], g.rxa.at[c, 1], g.sent.at[0], main.far_sem.at[(g.start + c) % RING], dp=at_x)

    def far_y(g, c):
        return remote(grad.at[at_d, rows_of(g, c), right], g.rxb.at[c, 1], g.sent.at[1], main.far_sem.at[(g.start + c) % RING], dp=at_y)

    def near_x(g, c):
        return remote(grad.at[at_x, rows_of(g, c), left], g.rxa.at[c, 0], g.sent.at[0], main.mid_sem.at[(g.start + c) % RING], dp=at_x)

    def near_y(g, c):
        return remote(grad.at[at_y, rows_of(g, c), right], g.rxb.at[c, 0], g.sent.at[1], main.mid_sem.at[(g.start + c) % RING], dp=at_y)

    def sum_y(g, c):
        return remote(g.txa.at[c], g.r2a.at[c], g.sent.at[2], main.mid_sem.at[(g.start + c) % RING], dp=at_y)

    def sum_x(g, c):
        return remote(g.txb.at[c], g.r2b.at[c], g.sent.at[2], main.mid_sem.at[(g.start + c) % RING], dp=at_x)

    def unit_y(g, c):
        return remote(g.ts.at[c, 0], g.rs.at[c, 0], g.sent.at[3], main.unit_sem.at[(g.start + c) % RING], dp=at_y)

    def unit_x(g, c):
        return remote(g.ts.at[c, 1], g.rs.at[c, 1], g.sent.at[3], main.unit_sem.at[(g.start + c) % RING], dp=at_x)

    def publish(g, c, hop):
        return remote(g.zs.at[c, hop - 1], g.zr.at[eng, hop, c], g.sent.at[4], main.z_sem.at[(g.start + c) % RING], tp=(tp + hop) % ranks)

    def forward(g, c, hop):
        block = g.zr.at[eng, hop, c]
        return remote(block, block, g.sent.at[5], main.f_sem.at[(g.start + c) % RING], eng=1 - eng)

    def wait_bytes(like, sem):
        pltpu.make_async_copy(like, like, sem).wait()

    def load_side(g, c):
        rows, sem = rows_of(g, c), g.load_sem.at[0, c % 2]
        return [
            pltpu.make_async_copy(grad.at[at_y, rows, left], g.side.at[c % 2, 0], sem),
            pltpu.make_async_copy(grad.at[at_x, rows, right], g.side.at[c % 2, 1], sem),
        ]

    def load_own(g, c):
        return [pltpu.make_async_copy(grad.at[me, rows_of(g, c)], g.own.at[c % 2], g.load_sem.at[1, c % 2])]

    def load_old(g, c):
        sem = g.load_sem.at[2, c % 2]
        return [pltpu.make_async_copy(states[i].at[rows_of(g, c)], g.old.at[c % 2, i], sem) for i in range(3)]

    def start(copies):
        for copy in copies:
            copy.start()

    pl.semaphore_wait(barrier, 2 + ranks)
    for c in range(FAR):
        start([far_x(main, c), far_y(main, c)])
        if c < NEAR:
            start([near_x(main, c), near_y(main, c)])
    for c in range(2):
        start(load_side(main, c) + load_own(main, c) + load_old(main, c))
    for c in range(2):
        start(load_side(tail, c) + load_own(tail, c) + load_old(tail, c))

    small = [
        pltpu.make_async_copy(rank_map_in, rank_map, small_sem.at[0]),
        pltpu.make_async_copy(adam_step_in, adam_step, small_sem.at[1]),
    ]
    start(small)
    for copy in small:
        copy.wait()
    count = jnp.full((1, 128), adam_step[0], jnp.int32).astype(jnp.float32)
    scale_one = 1.0 / (1.0 - jnp.exp(count * math.log(beta_one)))
    scale_two = 1.0 / (1.0 - jnp.exp(count * math.log(beta_two)))

    def reduce_side(g, c):
        slot = c % 2
        wait_bytes(g.side.at[slot], g.load_sem.at[0, slot])
        wait_bytes(g.rxa.at[c], main.far_sem.at[(g.start + c) % RING])
        pack_sum(g.side.at[slot, 0], g.rxa.at[c, 1], g.txa.at[c], g.ts.at[c, 0])
        start([sum_y(g, c), unit_y(g, c)])
        pack_sum(g.side.at[slot, 1], g.rxb.at[c, 1], g.txb.at[c], g.ts.at[c, 1])
        start([sum_x(g, c), unit_x(g, c)])

        @pl.when(c + 2 < g.chunks)
        def _():
            start(load_side(g, c + 2))

    def update(g, c):
        slot, rows = c % 2, rows_of(g, c)
        wait_bytes(g.own.at[slot], g.load_sem.at[1, slot])
        wait_bytes(g.old.at[slot], g.load_sem.at[2, slot])
        wait_bytes(g.own, main.mid_sem.at[(g.start + c) % RING])
        wait_bytes(g.rs.at[c], main.unit_sem.at[(g.start + c) % RING])

        def spread_out(value):
            return stacked(jnp.broadcast_to(value, (g.rows, 128)), STRIP // 128, 1)

        one, two = spread_out(scale_one), spread_out(scale_two)
        unit_a, unit_b = spread_out(g.rs[c, 0]), spread_out(g.rs[c, 1])
        for strip in range(columns // STRIP):
            at = pl.ds(strip * STRIP, STRIP)
            side = strip * STRIP // half
            inner = pl.ds(strip * STRIP - side * half, STRIP)
            got, sums, unit = ((g.rxa, g.r2a, unit_a), (g.rxb, g.r2b, unit_b))[side]
            summed = g.own[slot, :, at].astype(jnp.float32) + got[c, 0, :, inner].astype(jnp.float32)
            summed += sums[c, :, inner].astype(jnp.int32).astype(jnp.float32) * unit
            first_now = beta_one * g.old[slot, 1, :, at] + (1.0 - beta_one) * summed
            second_now = beta_two * g.old[slot, 2, :, at] + (1.0 - beta_two) * summed * summed
            was = g.old[slot, 0, :, at]
            step = (first_now * one) / (jnp.sqrt(second_now * two) + eps_value)
            now = was - rate_value * (step + decay_value * was)
            new_master[rows, at] = now
            new_first[rows, at] = first_now
            new_second[rows, at] = second_now
            block = strip * STRIP // width
            g.held[block, :, pl.ds(strip * STRIP - block * width, STRIP)] = now.astype(jnp.bfloat16)
        for hop in range(1, ranks):
            g.zs[c, hop - 1] = g.held[rank_map[(tp + hop) % ranks]]
            publish(g, c, hop).start()
        g.zr[eng, 0, c] = g.held[rank_map[tp]]
        forward(g, c, 0).start()

        @pl.when(c + 2 < g.chunks)
        def _():
            start(load_own(g, c + 2) + load_old(g, c + 2))

    def spread(g, c):
        wait_bytes(g.zs.at[c], main.z_sem.at[(g.start + c) % RING])
        for hop in range(1, ranks):
            forward(g, c, hop).start()

    def merge(g, c):
        wait_bytes(g.zr.at[1 - eng, :, c], main.f_sem.at[(g.start + c) % RING])
        for hop in range(ranks):
            for part in range(2):
                rollout[(tp + ranks - hop) % ranks, rows_of(g, c), part, :] = g.zr[part, hop, c]

    def at_step(s, lag, act):
        for g in (main, tail):
            c = s - lag - g.start

            @pl.when((c >= 0) & (c < g.chunks))
            def _():
                act(g, c)

    def send_far(g, c):
        start([far_x(g, c), far_y(g, c)])

    def send_near(g, c):
        start([near_x(g, c), near_y(g, c)])

    def body(s, carry):
        at_step(s, 0, reduce_side)
        at_step(s, -FAR, send_far)
        at_step(s, -NEAR, send_near)
        at_step(s, UPDATE, update)
        at_step(s, SPREAD, spread)
        at_step(s, MERGE, merge)
        return carry

    lax.fori_loop(0, main.chunks + tail.chunks + MERGE, body, 0)
    for g in (main, tail):
        for i, like in enumerate((g.rxa, g.rxb, g.rxa, g.ts, g.zs, g.zr.at[eng])):
            wait_bytes(like, g.sent.at[i])


def flush(*refs):
    count = (len(refs) - 1) // 2
    copies = [pltpu.make_async_copy(refs[i], refs[count + i], refs[-1].at[i]) for i in range(count)]
    for copy in copies:
        copy.start()
    for copy in copies:
        copy.wait()


def shards(grad_parts, master, first_moment, second_moment, adam_step, rank_map):
    replicas, ranks = lax.axis_size("dp"), lax.axis_size("tp")
    row_count, columns = master.shape[1], master.shape[2]
    half, width = columns // 2, columns // ranks
    grad = grad_parts.reshape(replicas, row_count, columns)
    states = [s.reshape(row_count, columns) for s in (master, first_moment, second_moment)]
    anywhere = pl.BlockSpec(memory_space=pl.ANY)
    vmem, dma = pltpu.VMEM, pltpu.SemaphoreType.DMA
    short, brain, single = jnp.int16, jnp.bfloat16, jnp.float32

    def scratch(chunks, rows):
        shapes = {name: vmem((chunks, 2, rows, half), brain) for name in ("rxa", "rxb")}
        shapes |= {name: vmem((chunks, rows, half), short) for name in ("txa", "txb", "r2a", "r2b")}
        shapes |= {name: vmem((chunks, 2, 1, 128), single) for name in ("ts", "rs")}
        shapes["zs"] = vmem((chunks, ranks - 1, rows, width), brain)
        shapes["zr"] = vmem((2, ranks, chunks, rows, width), brain)
        shapes["own"] = vmem((2, rows, columns), brain)
        shapes["side"] = vmem((2, 2, rows, half), brain)
        shapes["old"] = vmem((2, 3, rows, columns), single)
        shapes["held"] = vmem((ranks, rows, width), brain)
        shapes |= {name: dma((min(chunks, RING),)) for name in ("far_sem", "mid_sem", "unit_sem", "z_sem", "f_sem")}
        shapes["sent"] = dma((6,))
        shapes["load_sem"] = dma((3, 2))
        return shapes

    main = scratch(row_count // ROWS - 2, ROWS)
    tail = scratch(2 * ROWS // TAIL, TAIL)
    tail |= {name: dma((1,)) for name in ("far_sem", "mid_sem", "unit_sem", "z_sem", "f_sem")}
    results = pl.pallas_call(
        functools.partial(kernel, ranks, tuple(main)),
        out_shape=[vmem(s.shape, s.dtype) for s in states] + [vmem((ranks, row_count, 2, width), brain)],
        in_specs=[anywhere] * 6,
        out_specs=[pl.BlockSpec(memory_space=pltpu.VMEM)] * 4,
        scratch_shapes=[
            pltpu.SMEM(rank_map.shape, rank_map.dtype),
            pltpu.SMEM(adam_step.shape, adam_step.dtype),
            dma((2,)),
            *main.values(),
            *tail.values(),
        ],
        compiler_params=pltpu.CompilerParams(
            collective_id=0, has_side_effects=True, vmem_limit_bytes=34 * 1024 * 1024
        ),
        name="exchange",
    )(rank_map, adam_step, grad, *states)
    *outs, rollout = pl.pallas_call(
        flush,
        out_shape=[jax.ShapeDtypeStruct(r.shape, r.dtype) for r in results],
        in_specs=[anywhere] * 4,
        out_specs=[anywhere] * 4,
        scratch_shapes=[dma((4,))],
        compiler_params=pltpu.CompilerParams(vmem_limit_bytes=1024 * 1024),
        name="flush",
    )(*results)
    return (*(o.reshape(master.shape) for o in outs), rollout.reshape(ranks, row_count, 2, 1, width))


def solution(mesh):
    sizes = dict(mesh.shape)

    def step(grad_parts, master, *rest):
        columns = master.shape[2] // sizes["eng"]
        width = columns // sizes["tp"]
        rows = master.shape[1] // sizes["dp"]
        fits = sizes["dp"] == 4 and sizes["eng"] == 2 and width % STRIP == 0 and (columns // 2) % STRIP == 0
        fits = fits and rows % ROWS == 0 and rows // ROWS > FAR + 2
        return jax.shard_map(
            shards if fits else plain_shards,
            mesh=mesh,
            in_specs=(
                P("dp", "tp", None, "eng"),
                P("tp", "dp", "eng"),
                P("tp", "dp", "eng"),
                P("tp", "dp", "eng"),
                P(),
                P(),
            ),
            out_specs=(
                P("tp", "dp", "eng"),
                P("tp", "dp", "eng"),
                P("tp", "dp", "eng"),
                P(None, "dp", None, "tp", None),
            ),
            check_vma=False,
        )(grad_parts, master, *rest)

    return step
```
